32 devices in a mesh: env: 16 (over z, y, x), feat: 2 (over core).
Axes of the slice: x: 2, y: 2, z: 4, core: 2. Of those that a mesh axis runs over, the one named last changes fastest.
Arguments:
- observations: bfloat16 [8192, 8192], P('env', 'feat'), may hold values from -256 to 256, as said below
- prior_count: int32 [8192], P('feat'), may hold values from 2048 to 32767
- prior_mean: float32 [8192], P('feat'), may hold values from -12 to 12
- prior_var: float32 [8192], P('feat'), may hold values from 0.5 to 40
- policy_weight: bfloat16 [8192, 4096], P('feat', 'env'), may hold values from -0.0625 to 0.0625
Outputs:
- run_mean: float32 [8192], P('feat')
- run_var: float32 [8192], P('feat')
- logits: bfloat16 [8192, 4096], P('env', 'feat')
The draws below stay inside these ranges and needn't reach their ends.
Inputs may be any that keep to these rules, and one draw needn't show every extreme that they name: observations have per-environment scales and per-feature offsets.
All inputs are finite; a program needn't handle non-finite values.
Results may differ from the reference program's by a relative error of at most 0.013.
Values may be sent and summed in bfloat16 or wider, within the bound.
A program may use at most 128 MiB of HBM per device.

```python
import math
import jax
import jax.numpy as jnp
from jax import lax

D = 8192
H = 4096
TOKENS = 8192
N_FEAT = 2


def draw_observations(key, part):
    keys = jax.random.split(key, 4)
    rows = jnp.arange(TOKENS, dtype=jnp.float32)
    row_scale = jnp.exp(jax.random.uniform(keys[0], (TOKENS,), jnp.float32) * jnp.log(10.0)) * jnp.exp(jnp.log(3.0) * rows / TOKENS)
    feature_scale = jnp.exp(jax.random.uniform(keys[1], (D,), jnp.float32, -0.7, 0.7))
    offset = jax.random.normal(keys[2], (D,), jnp.float32)
    noise = jnp.clip(jax.random.normal(keys[3], (TOKENS, D), jnp.float32), -4.0, 4.0)
    values = offset[None, :] + row_scale[:, None] * feature_scale[None, :] * noise
    return jnp.clip(values, -256.0, 256.0).astype(jnp.bfloat16)


def with_ends(drawn, own_key, least, largest):
    dims = drawn.shape
    spot = [jax.random.randint(jax.random.fold_in(own_key, axis), (), 0, dims[axis]) for axis in range(len(dims))]
    drawn = drawn.at[tuple(spot)].set(least)
    longest = dims.index(max(dims))
    spot[longest] = (spot[longest] + 1) % dims[longest]
    return drawn.at[tuple(spot)].set(largest)


def level_of(key, shape, cuts, least, high):
    level, own = 1.0, jax.random.fold_in(key, 6)
    for dim, parts in cuts:
        draws = jnp.exp(jax.random.uniform(jax.random.fold_in(own, dim), (parts,), jnp.float32, least / len(cuts), high / len(cuts)))
        level = level * jnp.repeat(draws, shape[dim] // parts).reshape([-1 if axis == dim else 1 for axis in range(len(shape))])
    return level


def bell_draw(own_key, extent, spread, reach, shards=(), held_as=jnp.bfloat16):
    values = jax.random.normal(own_key, extent, jnp.float32) * spread
    if len(shards) > 0:
        values = level_of(own_key, extent, shards, -0.22, 0.18) * values
    return jnp.clip(values, min=-reach, max=reach).astype(held_as)


def setup_inputs(seed: int = 0) -> dict:
    key_of = jax.random.split(jax.random.key(seed), 6)
    observations = draw_observations(jax.random.fold_in(key_of[5], 71), 0)
    prior_count = with_ends(jax.random.randint(key_of[1], (D,), TOKENS // 4, 4 * TOKENS), jax.random.fold_in(key_of[1], 1), TOKENS // 4, (4 * TOKENS) - 1).astype(jnp.int32)
    prior_mean = bell_draw(key_of[2], (D,), 2.0, 12.0, ((0, 2),), jnp.float32)
    prior_var = jnp.clip(jnp.exp(math.log(40.0) - 4.3820266 * jax.random.uniform(key_of[3], (D,), jnp.float32) ** level_of(key_of[3], (D,), ((0, 2),), -0.2, 0.2)), 0.5, 40.0)
    policy_weight = bell_draw(key_of[4], (D, H), D ** -0.5, 0.0625, ((0, 2), (1, 16)))
    return dict(observations=observations, prior_count=prior_count, prior_mean=prior_mean, prior_var=prior_var, policy_weight=policy_weight)


def reference(observations, prior_count, prior_mean, prior_var, policy_weight):
    values = observations.astype(jnp.float32)
    batch_mean = lax.optimization_barrier(jnp.mean(values, axis=0))
    batch_m2 = lax.optimization_barrier(jnp.sum((values - batch_mean) ** 2, axis=0))
    count = prior_count.astype(jnp.float32)
    batch_n = jnp.float32(TOKENS)
    total = count + batch_n
    delta = batch_mean - prior_mean
    run_mean = prior_mean + delta * batch_n / total
    run_var = (prior_var * count + batch_m2 + delta * delta * count * batch_n / total) / total
    normalized = jnp.clip((values - run_mean) / jnp.sqrt(run_var + 1e-05), -5.0, 5.0).astype(jnp.bfloat16)
    width = D // N_FEAT
    summed = jnp.zeros((TOKENS, H), jnp.float32)
    for block in range(N_FEAT):
        left = normalized[:, block * width:(block + 1) * width].astype(jnp.float32)
        right = policy_weight[block * width:(block + 1) * width].astype(jnp.float32)
        partial_block = jnp.dot(left, right, precision=lax.Precision.HIGHEST).astype(jnp.bfloat16)
        summed = summed + partial_block.astype(jnp.float32)
    return (run_mean, run_var, summed.astype(jnp.bfloat16))
```

```python
import functools
import jax
import jax.numpy as jnp
from jax import lax
from jax.experimental import pallas as pl
from jax.experimental.pallas import tpu as pltpu
from jax.sharding import PartitionSpec as P

MESH = pl.DeviceIdType.MESH
CUTS = 4
AHEAD = 2


def shards_general(observations, prior_count, prior_mean, prior_var, policy_weight):
    rows = observations.shape[0]
    values = observations.astype(jnp.float32)
    batch_n = jnp.float32(rows * lax.axis_size("env"))
    local_mean = jnp.mean(values, axis=0)
    local_sq = jnp.sum((values - local_mean) ** 2, axis=0)
    batch_mean = lax.psum(jnp.sum(values, axis=0), "env") / batch_n
    shifted = local_sq + float(rows) * (local_mean - batch_mean) ** 2
    batch_m2 = lax.psum(shifted, "env")
    count = prior_count.astype(jnp.float32)
    total = count + batch_n
    delta = batch_mean - prior_mean
    run_mean = prior_mean + delta * batch_n / total
    run_var = (prior_var * count + batch_m2 + delta * delta * count * batch_n / total) / total
    normalized = jnp.clip((values - run_mean) / jnp.sqrt(run_var + 1e-05), -5.0, 5.0).astype(
        jnp.bfloat16
    )
    partial_block = jnp.dot(
        normalized,
        lax.all_gather(policy_weight, "env", axis=1, tiled=True),
        preferred_element_type=jnp.float32,
    ).astype(jnp.bfloat16)
    summed = lax.psum_scatter(partial_block, "feat", scatter_dimension=1, tiled=True)
    return (run_mean, run_var, summed)


def kernel(
    nz, obs, cnt, pmean, pvar, w, mean_out, var_out, out,
    X, Xn, Wb, Pb, R, F, A, S0, RX, S1, RY, RZ, NS, NP,
    loc, wloc, xs, xr, ds, ls, ys, rs, x3, d3, d1, d2, ws, wr, wq, wys, ss, sr, nsnd, nrcv, ps, pr, os_, orr, psl, prl, osl,
):
    rows, depth = obs.shape
    cols = w.shape[1]
    quarter = rows // 4
    half = cols // 2
    nblk = nz * 4
    env = lax.axis_index("env")
    f = lax.axis_index("feat")
    x = lax.rem(env, 2)
    y = lax.rem(env // 2, 2)
    z = env // 4
    ex = env + 1 - 2 * x
    ey = env + 2 - 4 * y
    sib = (env, 1 - f)
    native = f == y
    foreign = f != y
    pending = []

    def when(cond, fn):
        if cond is True:
            fn()
        else:
            pl.when(cond)(fn)

    def send(cond, make):
        when(cond, lambda: make().start())
        pending.append((cond, make))

    def rc(src, dst, s, r, dev):
        return pltpu.make_async_remote_copy(
            src_ref=src, dst_ref=dst, send_sem=s, recv_sem=r, device_id=dev, device_id_type=MESH
        )

    def arrived(dst, sem):
        pltpu.make_async_copy(dst, dst, sem).wait()

    def rq(ch):
        return pl.ds(ch * quarter, quarter)

    barrier = pltpu.get_barrier_semaphore()

    def greet(dev):
        pl.semaphore_signal(barrier, inc=1, device_id=dev, device_id_type=MESH)

    greet(sib)
    for g in range(2):
        greet((ex, g))
        greet((ey, g))
    for s in range(1, nz):
        greet((lax.rem(env + 4 * s, nblk), f))
    pl.semaphore_wait(barrier, 5 + nz - 1)

    stat_load = pltpu.make_async_copy(obs, Xn.at[0], loc.at[0])
    stat_load.start()
    w_load = pltpu.make_async_copy(w, Wb.at[z], wloc)
    when(native, lambda: w_load.start())
    own_load = pltpu.make_async_copy(obs, X.at[0], loc.at[1])
    when(native, lambda: own_load.start())

    def wk(h):
        return pl.ds(h * half, half)

    def own_w(h):
        send(foreign, lambda: rc(
            w.at[:, wk(h)], Wb.at[z, :, wk(h)], wys.at[h], wr.at[z, h], (ey, f_of_y(y))))

    own_w(0)

    def own_x(ch):
        dst_core = y if ch < 2 else 1 - y
        send(native, lambda: rc(obs.at[rq(ch)], X.at[1, rq(ch)], xs.at[ch], xr.at[1, ch], (ex, dst_core)))

    def own_y(ch):
        dst_core = 1 - y if ch < 2 else y
        send(foreign, lambda: rc(obs.at[rq(ch)], X.at[2, rq(ch)], ys.at[ch], xr.at[2, ch], (ey, dst_core)))

    zup = z + 1 < nz
    zdn = z >= 1
    for h in range(2):
        when(native & zup, lambda h=h: rc(
            w.at[:, wk(h)], Wb.at[z, :, wk(h)], ws.at[0, 0, h], wr.at[z, h], (env + 4, f)).start())
        when(native & zdn, lambda h=h: rc(
            w.at[:, wk(h)], Wb.at[z, :, wk(h)], ws.at[1, 0, h], wr.at[z, h], (env - 4, f)).start())
    own_x(0)

    kcut = depth // CUTS

    def cut(h, q):
        kq = pl.ds(q * kcut, kcut)
        far_s = nz - 2

        def part(t, dev):
            return rc(Wb.at[t, kq, wk(h)], Wb.at[t, kq, wk(h)], wq.at[0, h, q], wq.at[1, h, q], dev)

        return (
            ((z - far_s >= 0) & (z + 1 < nz), lambda: part(z - far_s, (env + 4, f))),
            ((z + far_s < nz) & (z >= 1), lambda: part(z + far_s, (env - 4, f))),
        )

    def cut_start(h, q):
        for c, make in cut(h, q):
            when(foreign & c, lambda make=make: make().start())

    def cut_sent(h, q):
        for c, make in cut(h, q):
            when(foreign & c, lambda make=make: make().wait_send())

    flow = [(h, q) for h in range(2) for q in range(CUTS)]

    def zsend(s, h, who):
        up = who & (z - s >= 0) & (z + 1 < nz)
        down = who & (z + s < nz) & (z >= 1)
        if s == nz - 2:
            for q in range(CUTS):
                for c, make in cut(h, q):
                    send(who & c, make)
            return
        send(up, lambda: rc(
            Wb.at[z - s, :, wk(h)], Wb.at[z - s, :, wk(h)], ws.at[0, s, h], wr.at[z - s, h], (env + 4, f)))
        send(down, lambda: rc(
            Wb.at[z + s, :, wk(h)], Wb.at[z + s, :, wk(h)], ws.at[1, s, h], wr.at[z + s, h], (env - 4, f)))

    def zrecv(s, h, who=True):
        when(who & (z - 1 - s >= 0), lambda: arrived(Wb.at[z - 1 - s, :, wk(h)], wr.at[z - 1 - s, h]))
        when(who & (z + 1 + s < nz), lambda: arrived(Wb.at[z + 1 + s, :, wk(h)], wr.at[z + 1 + s, h]))

    stat_load.wait()
    tile = 512
    strip = 32

    def moments(c, carry):
        cs = pl.ds(pl.multiple_of(c * tile, tile), tile)

        def add(i, acc):
            v = Xn[0, pl.ds(pl.multiple_of(i * strip, strip), strip), cs].astype(jnp.float32)
            return acc + v.reshape(strip // 8, 8, tile).sum(0)

        tot = lax.fori_loop(0, rows // strip, add, jnp.zeros((8, tile), jnp.float32))
        mean = jnp.sum(tot, axis=0, keepdims=True) * (1.0 / rows)

        def add2(i, acc):
            v = Xn[0, pl.ds(pl.multiple_of(i * strip, strip), strip), cs].astype(jnp.float32) - mean
            return acc + (v * v).reshape(strip // 8, 8, tile).sum(0)

        tot2 = lax.fori_loop(0, rows // strip, add2, jnp.zeros((8, tile), jnp.float32))
        S0[0:1, cs] = mean
        S0[1:2, cs] = jnp.sum(tot2, axis=0, keepdims=True)
        return carry

    lax.fori_loop(0, depth // tile, moments, 0)
    send(True, lambda: rc(S0, RX, ss.at[0], sr.at[0], (ex, f)))
    for ch in (2, 1):
        own_x(ch)
    arrived(RX, sr.at[0])
    m0, m1 = S0[0:1, :], RX[0:1, :]
    S1[0:1, :] = 0.5 * (m0 + m1)
    S1[1:2, :] = S0[1:2, :] + RX[1:2, :] + (0.5 * rows) * (m0 - m1) * (m0 - m1)
    send(True, lambda: rc(S1, RY, ss.at[1], sr.at[1], (ey, f)))
    own_w(1)
    for ch in (0, 2, 1, 3):
        own_y(ch)
    send(native, lambda: rc(obs, X.at[0], ds, xr.at[0, 0], sib))

    def base(h):
        def fn():
            arrived(Wb.at[z, :, wk(h)], wr.at[z, h])

            @pl.when(zup)
            def _():
                rc(Wb.at[z, :, wk(h)], Wb.at[z, :, wk(h)], ws.at[0, 0, h], wr.at[z, h], (env + 4, f)).start()

            @pl.when(zdn)
            def _():
                rc(Wb.at[z, :, wk(h)], Wb.at[z, :, wk(h)], ws.at[1, 0, h], wr.at[z, h], (env - 4, f)).start()

        when(foreign, fn)
        pending.append((zup, lambda: rc(
            Wb.at[z, :, wk(h)], Wb.at[z, :, wk(h)], ws.at[0, 0, h], wr.at[z, h], (env + 4, f))))
        pending.append((zdn, lambda: rc(
            Wb.at[z, :, wk(h)], Wb.at[z, :, wk(h)], ws.at[1, 0, h], wr.at[z, h], (env - 4, f))))

    base(0)
    arrived(RY, sr.at[1])
    m0, m1 = S1[0:1, :], RY[0:1, :]
    RZ[z, 0:1, :] = 0.5 * (m0 + m1)
    RZ[z, 1:2, :] = S1[1:2, :] + RY[1:2, :] + (1.0 * rows) * (m0 - m1) * (m0 - m1)
    for s in range(1, nz):
        send(True, lambda s=s: rc(
            RZ.at[z], RZ.at[z], ss.at[1 + s], sr.at[2 + z], (lax.rem(env + 4 * s, nblk), f)))
    base(1)

    lb = jnp.where(native, 0, 2)

    def land(b, i, who):
        ch = lb + i
        sl = pl.ds(pl.multiple_of(ch * quarter, quarter), quarter)
        when(who, lambda: arrived(X.at[b, sl], xr.at[b, ch]))
        sem = {1: d1, 2: d2, 3: d3}[b]
        if b == 2:
            send(who, lambda: rc(X.at[2, sl], X.at[3, sl], x3.at[i], xr.at[3, ch], (ex, f)))
        send(who, lambda: rc(X.at[b, sl], X.at[b, sl], sem.at[i], xr.at[b, ch], sib))

    def relay(s, h, who):
        zrecv(s, h, who)
        if s + 1 < nz - 1:
            zsend(s + 1, h, who)

    relay(0, 0, native)
    relay(0, 1, native)
    land(2, 0, native)
    land(1, 0, native)
    land(1, 1, native)
    land(1, 0, foreign)
    relay(0, 0, foreign)
    land(2, 0, foreign)

    for s in range(1, nz):
        o = lax.rem(z + s, nz)
        arrived(RZ.at[o], sr.at[2 + o])
    bmean = RZ[0, 0:1, :]
    for o in range(1, nz):
        bmean = bmean + RZ[o, 0:1, :]
    bmean = bmean * (1.0 / nz)
    m2 = jnp.zeros_like(bmean)
    per = float(rows * 4)
    for o in range(nz):
        dev = RZ[o, 0:1, :] - bmean
        m2 = m2 + RZ[o, 1:2, :] + per * dev * dev
    batch_n = float(rows * nblk)
    count = cnt[...].astype(jnp.float32)
    total = count + batch_n
    delta = bmean - pmean[...]
    new_mean = pmean[...] + delta * batch_n / total
    new_var = (pvar[...] * count + m2 + delta * delta * count * batch_n / total) / total
    mean_out[...] = new_mean
    var_out[...] = new_var
    NS[0:1, :] = new_mean
    NS[1:2, :] = 1.0 / jnp.sqrt(new_var + 1e-05)

    @pl.when(native)
    def _():
        NP[...] = NS[...]

    send(native, lambda: rc(NS, NP, nsnd, nrcv, sib))
    when(foreign, lambda: arrived(NP, nrcv))

    def normalize(b):
        def step(i, carry):
            c = i // (rows // 32)
            r = lax.rem(i, rows // 32)
            cs = pl.ds(pl.multiple_of(c * 1024, 1024), 1024)
            sl = pl.ds(pl.multiple_of(r * 32, 32), 32)
            v = X[b, sl, cs].astype(jnp.float32)
            v = (v - NP[0:1, cs]) * NP[1:2, cs]
            Xn[b, sl, cs] = jnp.clip(v, -5.0, 5.0).astype(jnp.bfloat16)
            return carry

        lax.fori_loop(0, (rows // 32) * (depth // 1024), step, 0)

    def rest(b):
        for i in range(2):
            ch = 2 - lb + i
            sl = pl.ds(pl.multiple_of(ch * quarter, quarter), quarter)
            arrived(X.at[b, sl], xr.at[b, ch])

    mt = 256

    def matmul(t, b0, b1):
        def step(i, carry):
            b = b0 + i // (rows // mt)
            sl = pl.ds(pl.multiple_of(lax.rem(i, rows // mt) * mt, mt), mt)
            Pb[t, b, sl, :] = jnp.dot(
                Xn[b, sl, :], Wb[t], preferred_element_type=jnp.float32
            ).astype(jnp.bfloat16)
            return carry

        lax.fori_loop(0, (b1 - b0) * (rows // mt), step, 0)

    def give(t, b, cond):
        send(cond, lambda: rc(Pb.at[t, b], R.at[t, b - 2], ps.at[t, b - 2], pr.at[t, b - 2], (ey, f)))

    own_cols = out.shape[1]

    def finish(t, b, cond):
        def fn():
            arrived(R.at[t, b], pr.at[t, b])

            def step(i, carry):
                sl = pl.ds(pl.multiple_of(i * 128, 128), 128)
                F[t, b, sl, :] = (
                    Pb[t, b, sl, :].astype(jnp.float32) + R[t, b, sl, :].astype(jnp.float32)
                ).astype(jnp.bfloat16)
                return carry

            lax.fori_loop(0, rows // 128, step, 0)

        when(cond, fn)
        core = t // (nz // 2)
        idx = lax.rem(t, nz // 2)
        at = (t * 4 + f * 2 + x) * cols - core * own_cols
        dst = out.at[:, pl.ds(pl.multiple_of(at, cols), cols)]
        if b == 1:
            send(cond, lambda: rc(F.at[t, 1], dst, os_.at[t, 0], orr.at[idx, 1 + f], (ex, core)))
            return
        send(cond & (core != f), lambda: rc(F.at[t, 0], dst, os_.at[t, 1], orr.at[idx, 0], sib))

        def keep():
            out[:, pl.ds(pl.multiple_of(at, cols), cols)] = F[t, 0]

        when(cond & (core == f), keep)

    def strips(s):
        if s == 0:
            return [(z, z >= 0)]
        return [(lax.max(z - s, 0), z - s >= 0), (lax.min(z + s, nz - 1), z + s < nz)]

    when(native, lambda: w_load.wait())
    when(native, lambda: own_load.wait())
    when(foreign, lambda: arrived(X.at[0], xr.at[0, 0]))
    normalize(0)
    matmul(z, 0, 1)
    relay(1, 0, native)
    land(2, 1, native)
    relay(0, 1, foreign)
    land(2, 1, foreign)
    rest(2)
    normalize(2)
    near = strips(0) + strips(1)

    def offer(group, b, who):
        for t, c in group:
            when(who & c, lambda t=t: matmul(t, b, b + 1))
            give(t, b, who & c)

    offer(near, 2, True)
    own_x(3)
    relay(1, 1, native)
    offer(strips(2), 2, native)
    zrecv(1, 0, foreign)
    for h, q in flow[:AHEAD]:
        cut_start(h, q)
    land(3, 0, True)
    land(3, 1, True)
    rest(3)
    normalize(3)
    offer(near, 3, True)
    offer(strips(2), 3, native)
    for t, c in near[1:]:
        when(c, lambda t=t: matmul(t, 0, 1))
    land(1, 1, foreign)
    rest(1)
    normalize(1)
    for t, c in near:
        when(c, lambda t=t: matmul(t, 1, 2))
    zrecv(1, 1, foreign)
    offer(strips(2), 3, foreign)
    offer(strips(2), 2, foreign)
    for t, c in strips(2):
        when(c, lambda t=t: matmul(t, 0, 2))
    for i in range(AHEAD, AHEAD + 2):
        cut_sent(*flow[i - AHEAD])
        cut_start(*flow[i])
    for t, c in near:
        finish(t, 0, c)
        finish(t, 1, c)
    for i in range(AHEAD + 2, len(flow)):
        cut_sent(*flow[i - AHEAD])
        cut_start(*flow[i])
    for h, q in flow[-AHEAD:]:
        for c, make in cut(h, q):
            pending.append((foreign & c, make))
    for t, c in strips(2):
        finish(t, 1, c)
        finish(t, 0, c)

    far = nz - 1 - z
    end = (z == 0) | (z == nz - 1)
    core = far // (nz // 2)
    idx = lax.rem(far, nz // 2)
    at = (far * 4 + f * 2 + x) * cols - core * own_cols
    np_ = rows // mt

    def piece(b, u, h):
        sl = pl.ds(u * mt, mt)
        kl = pl.ds(depth - kcut, kcut)

        def fn():
            Pb[far, b, sl, wk(h)] = (A[pl.ds(b * rows + u * mt, mt), :] + jnp.dot(
                Xn[b, sl, kl], Wb[far, kl, wk(h)], preferred_element_type=jnp.float32
            )).astype(jnp.bfloat16)

        when(end, fn)

    def gather(h):
        def step(q, carry):
            kq = pl.ds(pl.multiple_of(q * kcut, kcut), kcut)
            arrived(Wb.at[far, kq, wk(h)], wq.at[1, h, q])
            left = Xn[:, :, kq].reshape(4 * rows, kcut)
            A[...] += jnp.dot(left, Wb[far, kq, wk(h)], preferred_element_type=jnp.float32)
            return carry

        def fn():
            A[...] = jnp.zeros_like(A)
            lax.fori_loop(0, CUTS - 1, step, 0)
            arrived(Wb.at[far, pl.ds(depth - kcut, kcut), wk(h)], wq.at[1, h, CUTS - 1])

        when(end, fn)

    def pass_on(b, u, h):
        sl = pl.ds(u * mt, mt)
        k = (b - 2) * np_ + u
        send(end, lambda: rc(
            Pb.at[far, b, sl, wk(h)], R.at[far, b - 2, sl, wk(h)],
            psl.at[h, k], prl.at[h, k], (ey, f)))

    def settle(b, u, h):
        sl = pl.ds(u * mt, mt)
        k = b * np_ + u

        def fn():
            arrived(R.at[far, b, sl, wk(h)], prl.at[h, k])
            F[far, b, sl, wk(h)] = (
                Pb[far, b, sl, wk(h)].astype(jnp.float32) + R[far, b, sl, wk(h)].astype(jnp.float32)
            ).astype(jnp.bfloat16)

        when(end, fn)
        dst = out.at[sl, pl.ds(pl.multiple_of(at + h * half, half), half)]
        src = F.at[far, b, sl, wk(h)]
        if b == 1:
            send(end, lambda: rc(src, dst, osl.at[h, k], orr.at[idx, 1 + f], (ex, core)))
        else:
            send(end & (core != f), lambda: rc(src, dst, osl.at[h, k], orr.at[idx, 0], sib))

            def keep():
                out[sl, pl.ds(pl.multiple_of(at + h * half, half), half)] = F[far, b, sl, wk(h)]

            when(end & (core == f), keep)

    for h in range(2):
        gather(h)
        for b in (3, 2):
            for u in range(np_):
                piece(b, u, h)
                pass_on(b, u, h)
        for b in (1, 0):
            for u in range(np_):
                piece(b, u, h)
        for b in (1, 0):
            for u in range(np_):
                settle(b, u, h)

    for i in range(nz // 2):
        t = f * (nz // 2) + i
        for src in range(3):
            sf = 1 - f if src == 0 else src - 1
            sx = x if src == 0 else 1 - x
            at = (t * 4 + sf * 2 + sx) * cols - f * own_cols
            arrived(out.at[:, pl.ds(pl.multiple_of(at, cols), cols)], orr.at[i, src])
    for cond, make in pending:
        when(cond, lambda make=make: make().wait_send())


def f_of_y(y):
    return y


def shards_planes(nz, observations, prior_count, prior_mean, prior_var, policy_weight):
    rows, depth = observations.shape
    cols = policy_weight.shape[1]
    n = lax.axis_size("env")
    own_cols = cols * n // 2
    bf, f32 = jnp.bfloat16, jnp.float32
    dma = pltpu.SemaphoreType.DMA
    vmem = pl.BlockSpec(memory_space=pltpu.VMEM)
    hbm = pl.BlockSpec(memory_space=pl.ANY)
    scratch = [
        pltpu.VMEM((4, rows, depth), bf),
        pltpu.VMEM((4, rows, depth), bf),
        pltpu.VMEM((nz, depth, cols), bf),
        pltpu.VMEM((nz, 4, rows, cols), bf),
        pltpu.VMEM((nz, 2, rows, cols), bf),
        pltpu.VMEM((nz, 2, rows, cols), bf),
        pltpu.VMEM((4 * rows, cols // 2), f32),
        pltpu.VMEM((2, depth), f32),
        pltpu.VMEM((2, depth), f32),
        pltpu.VMEM((2, depth), f32),
        pltpu.VMEM((2, depth), f32),
        pltpu.VMEM((nz, 2, depth), f32),
        pltpu.VMEM((2, depth), f32),
        pltpu.VMEM((2, depth), f32),
        dma((2,)),
        dma,
        dma((4,)),
        dma((4, 4)),
        dma,
        dma,
        dma((4,)),
        dma,
        dma((2,)),
        dma((2,)),
        dma((2,)),
        dma((2,)),
        dma((2, nz, 2)),
        dma((nz, 2)),
        dma((2, 2, CUTS)),
        dma((2,)),
        dma((nz + 1,)),
        dma((nz + 2,)),
        dma,
        dma,
        dma((nz, 2)),
        dma((nz, 2)),
        dma((nz, 2)),
        dma((nz // 2, 3)),
        dma((2, rows // 128)),
        dma((2, rows // 128)),
        dma((2, rows // 128)),
    ]
    row = lambda a: a.reshape(1, depth)
    run_mean, run_var, logits = pl.pallas_call(
        functools.partial(kernel, nz),
        out_shape=(
            pltpu.VMEM((1, depth), f32),
            pltpu.VMEM((1, depth), f32),
            pltpu.VMEM((rows, own_cols), bf),
        ),
        in_specs=[hbm, vmem, vmem, vmem, hbm],
        out_specs=(vmem, vmem, vmem),
        scratch_shapes=scratch,
        compiler_params=pltpu.CompilerParams(
            collective_id=0, has_side_effects=True, vmem_limit_bytes=58 * 1024 * 1024
        ),
    )(observations, row(prior_count), row(prior_mean), row(prior_var), policy_weight)
    return run_mean.reshape(depth), run_var.reshape(depth), logits


def plane_count(mesh):
    devices = mesh.devices
    if devices.ndim != 2 or devices.shape[1] != 2 or devices.shape[0] % 8:
        return 0
    base = devices[0, 0].coords
    for i in range(devices.shape[0]):
        for j in range(2):
            at = [a - b for a, b in zip(devices[i, j].coords, base)]
            if at != [i % 2, i // 2 % 2, i // 4]:
                return 0
    return devices.shape[0] // 4


def solution(mesh):
    placed = (P("env", "feat"), P("feat"), P("feat"), P("feat"), P("feat", "env"))
    nz = plane_count(mesh)
    body = functools.partial(shards_planes, nz) if nz == 4 else shards_general
    return jax.shard_map(
        body,
        mesh=mesh,
        in_specs=placed,
        out_specs=(P("feat"), P("feat"), P("env", "feat")),
        check_vma=False,
    )
```

```python
import functools
import jax
import jax.numpy as jnp
from jax import lax
from jax.experimental import pallas as pl
from jax.experimental.pallas import tpu as pltpu
from jax.sharding import PartitionSpec as P

MESH = pl.DeviceIdType.MESH
CUTS = 4
AHEAD = 2


def shards_general(observations, prior_count, prior_mean, prior_var, policy_weight):
    rows = observations.shape[0]
    values = observations.astype(jnp.float32)
    batch_n = jnp.float32(rows * lax.axis_size("env"))
    local_mean = jnp.mean(values, axis=0)
    local_sq = jnp.sum((values - local_mean) ** 2, axis=0)
    batch_mean = lax.psum(jnp.sum(values, axis=0), "env") / batch_n
    shifted = local_sq + float(rows) * (local_mean - batch_mean) ** 2
    batch_m2 = lax.psum(shifted, "env")
    count = prior_count.astype(jnp.float32)
    total = count + batch_n
    delta = batch_mean - prior_mean
    run_mean = prior_mean + delta * batch_n / total
    run_var = (prior_var * count + batch_m2 + delta * delta * count * batch_n / total) / total
    normalized = jnp.clip((values - run_mean) / jnp.sqrt(run_var + 1e-05), -5.0, 5.0).astype(
        jnp.bfloat16
    )
    partial_block = jnp.dot(
        normalized,
        lax.all_gather(policy_weight, "env", axis=1, tiled=True),
        preferred_element_type=jnp.float32,
    ).astype(jnp.bfloat16)
    summed = lax.psum_scatter(partial_block, "feat", scatter_dimension=1, tiled=True)
    return (run_mean, run_var, summed)


def kernel(
    nz, obs, cnt_in, pmean_in, pvar_in, w, mean_out, var_out, out,
    X, Xn, Wb, Pb, R, F, A, E, cnt, pmean, pvar, S0, RX, S1, RY, RZ, NS, NP,
    loc, ploc, wloc, es, er, xs, xr, ds, ys, x3, d3, d1, d2, ws, wr, wq, wys, ss, sr, nsnd, nrcv, ps, pr, os_, orr, psl, prl, osl,
):
    rows, depth = obs.shape
    cols = w.shape[1]
    quarter = rows // 4
    half = cols // 2
    nblk = nz * 4
    env = lax.axis_index("env")
    f = lax.axis_index("feat")
    x = lax.rem(env, 2)
    y = lax.rem(env // 2, 2)
    z = env // 4
    ex = env + 1 - 2 * x
    ey = env + 2 - 4 * y
    sib = (env, 1 - f)
    native = f == y
    foreign = f != y
    pending = []

    def when(cond, fn):
        if cond is True:
            fn()
        else:
            pl.when(cond)(fn)

    def send(cond, make):
        when(cond, lambda: make().start())
        pending.append((cond, make))

    def rc(src, dst, s, r, dev):
        return pltpu.make_async_remote_copy(
            src_ref=src, dst_ref=dst, send_sem=s, recv_sem=r, device_id=dev, device_id_type=MESH
        )

    def arrived(dst, sem):
        pltpu.make_async_copy(dst, dst, sem).wait()

    def rq(ch):
        return pl.ds(ch * quarter, quarter)

    barrier = pltpu.get_barrier_semaphore()

    def greet(dev):
        pl.semaphore_signal(barrier, inc=1, device_id=dev, device_id_type=MESH)

    greet(sib)
    for g in range(2):
        greet((ex, g))
        greet((ey, g))
    for s in range(1, nz):
        greet((lax.rem(env + 4 * s, nblk), f))

    stat_load = pltpu.make_async_copy(obs, Xn.at[0], loc.at[0])
    stat_load.start()
    w_load = pltpu.make_async_copy(w, Wb.at[z], wloc)
    when(native, lambda: w_load.start())
    own_load = pltpu.make_async_copy(obs, X.at[0], loc.at[1])
    when(native, lambda: own_load.start())

    prior = [
        pltpu.make_async_copy(src, dst, ploc.at[i])
        for i, (src, dst) in enumerate(((cnt_in, cnt), (pmean_in, pmean), (pvar_in, pvar)))
    ]
    for copy in prior:
        copy.start()
    pl.semaphore_wait(barrier, 5 + nz - 1)

    def wk(h):
        return pl.ds(h * half, half)

    def own_w(h):
        send(foreign, lambda: rc(
            w.at[:, wk(h)], Wb.at[z, :, wk(h)], wys.at[h], wr.at[z, h], (ey, f_of_y(y))))

    own_w(0)

    def own_x(ch):
        dst_core = y if ch < 2 else 1 - y
        send(native, lambda: rc(obs.at[rq(ch)], X.at[1, rq(ch)], xs.at[ch], xr.at[1, ch], (ex, dst_core)))

    def own_y(ch):
        dst_core = 1 - y if ch < 2 else y
        send(foreign, lambda: rc(obs.at[rq(ch)], X.at[2, rq(ch)], ys.at[ch], xr.at[2, ch], (ey, dst_core)))

    zup = z + 1 < nz
    zdn = z >= 1
    for h in range(2):
        when(native & zup, lambda h=h: rc(
            w.at[:, wk(h)], Wb.at[z, :, wk(h)], ws.at[0, 0, h], wr.at[z, h], (env + 4, f)).start())
        when(native & zdn, lambda h=h: rc(
            w.at[:, wk(h)], Wb.at[z, :, wk(h)], ws.at[1, 0, h], wr.at[z, h], (env - 4, f)).start())
    own_x(0)

    kcut = depth // CUTS

    def cut(h, q):
        kq = pl.ds(q * kcut, kcut)
        far_s = nz - 2

        def part(t, dev):
            return rc(Wb.at[t, kq, wk(h)], Wb.at[t, kq, wk(h)], wq.at[0, h, q], wq.at[1, h, q], dev)

        return (
            ((z - far_s >= 0) & (z + 1 < nz), lambda: part(z - far_s, (env + 4, f))),
            ((z + far_s < nz) & (z >= 1), lambda: part(z + far_s, (env - 4, f))),
        )

    def cut_start(h, q):
        for c, make in cut(h, q):
            when(foreign & c, lambda make=make: make().start())

    def cut_sent(h, q):
        for c, make in cut(h, q):
            when(foreign & c, lambda make=make: make().wait_send())

    flow = [(h, q) for h in range(2) for q in range(CUTS)]

    def zsend(s, h, who):
        up = who & (z - s >= 0) & (z + 1 < nz)
        down = who & (z + s < nz) & (z >= 1)
        if s == nz - 2:
            for q in range(CUTS):
                for c, make in cut(h, q):
                    send(who & c, make)
            return
        send(up, lambda: rc(
            Wb.at[z - s, :, wk(h)], Wb.at[z - s, :, wk(h)], ws.at[0, s, h], wr.at[z - s, h], (env + 4, f)))
        send(down, lambda: rc(
            Wb.at[z + s, :, wk(h)], Wb.at[z + s, :, wk(h)], ws.at[1, s, h], wr.at[z + s, h], (env - 4, f)))

    def zrecv(s, h, who=True):
        when(who & (z - 1 - s >= 0), lambda: arrived(Wb.at[z - 1 - s, :, wk(h)], wr.at[z - 1 - s, h]))
        when(who & (z + 1 + s < nz), lambda: arrived(Wb.at[z + 1 + s, :, wk(h)], wr.at[z + 1 + s, h]))

    stat_load.wait()
    tile = 512
    strip = 32

    def moments(c, carry):
        cs = pl.ds(pl.multiple_of(c * tile, tile), tile)

        def add(i, acc):
            v = Xn[0, pl.ds(pl.multiple_of(i * strip, strip), strip), cs].astype(jnp.float32)
            return acc + v.reshape(strip // 8, 8, tile).sum(0)

        tot = lax.fori_loop(0, rows // strip, add, jnp.zeros((8, tile), jnp.float32))
        mean = jnp.sum(tot, axis=0, keepdims=True) * (1.0 / rows)

        def add2(i, acc):
            v = Xn[0, pl.ds(pl.multiple_of(i * strip, strip), strip), cs].astype(jnp.float32) - mean
            return acc + (v * v).reshape(strip // 8, 8, tile).sum(0)

        tot2 = lax.fori_loop(0, rows // strip, add2, jnp.zeros((8, tile), jnp.float32))
        S0[0:1, cs] = mean
        S0[1:2, cs] = jnp.sum(tot2, axis=0, keepdims=True)
        return carry

    lax.fori_loop(0, depth // tile, moments, 0)
    send(True, lambda: rc(S0, RX, ss.at[0], sr.at[0], (ex, f)))
    for ch in (2, 1):
        own_x(ch)
    arrived(RX, sr.at[0])
    m0, m1 = S0[0:1, :], RX[0:1, :]
    S1[0:1, :] = 0.5 * (m0 + m1)
    S1[1:2, :] = S0[1:2, :] + RX[1:2, :] + (0.5 * rows) * (m0 - m1) * (m0 - m1)
    send(True, lambda: rc(S1, RY, ss.at[1], sr.at[1], (ey, f)))
    own_w(1)
    for ch in (0, 2, 1, 3):
        own_y(ch)
    send(native, lambda: rc(obs, X.at[0], ds, xr.at[0, 0], sib))

    def base(h):
        def fn():
            arrived(Wb.at[z, :, wk(h)], wr.at[z, h])

            @pl.when(zup)
            def _():
                rc(Wb.at[z, :, wk(h)], Wb.at[z, :, wk(h)], ws.at[0, 0, h], wr.at[z, h], (env + 4, f)).start()

            @pl.when(zdn)
            def _():
                rc(Wb.at[z, :, wk(h)], Wb.at[z, :, wk(h)], ws.at[1, 0, h], wr.at[z, h], (env - 4, f)).start()

        when(foreign, fn)
        pending.append((zup, lambda: rc(
            Wb.at[z, :, wk(h)], Wb.at[z, :, wk(h)], ws.at[0, 0, h], wr.at[z, h], (env + 4, f))))
        pending.append((zdn, lambda: rc(
            Wb.at[z, :, wk(h)], Wb.at[z, :, wk(h)], ws.at[1, 0, h], wr.at[z, h], (env - 4, f))))

    base(0)
    arrived(RY, sr.at[1])
    m0, m1 = S1[0:1, :], RY[0:1, :]
    RZ[z, 0:1, :] = 0.5 * (m0 + m1)
    RZ[z, 1:2, :] = S1[1:2, :] + RY[1:2, :] + (1.0 * rows) * (m0 - m1) * (m0 - m1)
    for s in range(1, nz):
        send(True, lambda s=s: rc(
            RZ.at[z], RZ.at[z], ss.at[1 + s], sr.at[2 + z], (lax.rem(env + 4 * s, nblk), f)))
    base(1)

    lb = jnp.where(native, 0, 2)

    def land(b, i, who):
        ch = lb + i
        sl = pl.ds(pl.multiple_of(ch * quarter, quarter), quarter)
        when(who, lambda: arrived(X.at[b, sl], xr.at[b, ch]))
        sem = {1: d1, 2: d2, 3: d3}[b]
        if b == 2:
            send(who, lambda: rc(X.at[2, sl], X.at[3, sl], x3.at[i], xr.at[3, ch], (ex, f)))
        send(who, lambda: rc(X.at[b, sl], X.at[b, sl], sem.at[i], xr.at[b, ch], sib))

    def relay(s, h, who):
        zrecv(s, h, who)
        if s + 1 < nz - 1:
            zsend(s + 1, h, who)

    relay(0, 0, native)
    relay(0, 1, native)
    land(2, 0, native)
    land(1, 0, native)
    land(1, 1, native)
    land(1, 0, foreign)
    relay(0, 0, foreign)
    land(2, 0, foreign)

    for s in range(1, nz):
        o = lax.rem(z + s, nz)
        arrived(RZ.at[o], sr.at[2 + o])
    bmean = RZ[0, 0:1, :]
    for o in range(1, nz):
        bmean = bmean + RZ[o, 0:1, :]
    bmean = bmean * (1.0 / nz)
    m2 = jnp.zeros_like(bmean)
    per = float(rows * 4)
    for o in range(nz):
        dev = RZ[o, 0:1, :] - bmean
        m2 = m2 + RZ[o, 1:2, :] + per * dev * dev
    batch_n = float(rows * nblk)
    for copy in prior:
        copy.wait()
    count = cnt[...].astype(jnp.float32)
    total = count + batch_n
    delta = bmean - pmean[...]
    new_mean = pmean[...] + delta * batch_n / total
    new_var = (pvar[...] * count + m2 + delta * delta * count * batch_n / total) / total
    mean_out[...] = new_mean
    var_out[...] = new_var
    NS[0:1, :] = new_mean
    NS[1:2, :] = 1.0 / jnp.sqrt(new_var + 1e-05)

    @pl.when(native)
    def _():
        NP[...] = NS[...]

    send(native, lambda: rc(NS, NP, nsnd, nrcv, sib))
    when(foreign, lambda: arrived(NP, nrcv))

    def normalize(b):
        def step(i, carry):
            c = i // (rows // 32)
            r = lax.rem(i, rows // 32)
            cs = pl.ds(pl.multiple_of(c * 1024, 1024), 1024)
            sl = pl.ds(pl.multiple_of(r * 32, 32), 32)
            v = X[b, sl, cs].astype(jnp.float32)
            v = (v - NP[0:1, cs]) * NP[1:2, cs]
            Xn[b, sl, cs] = jnp.clip(v, -5.0, 5.0).astype(jnp.bfloat16)
            return carry

        lax.fori_loop(0, (rows // 32) * (depth // 1024), step, 0)

    def rest(b):
        for i in range(2):
            ch = 2 - lb + i
            sl = pl.ds(pl.multiple_of(ch * quarter, quarter), quarter)
            arrived(X.at[b, sl], xr.at[b, ch])

    mt = 256

    def matmul(t, b0, b1):
        def step(i, carry):
            b = b0 + i // (rows // mt)
            sl = pl.ds(pl.multiple_of(lax.rem(i, rows // mt) * mt, mt), mt)
            Pb[t, b, sl, :] = jnp.dot(
                Xn[b, sl, :], Wb[t], preferred_element_type=jnp.float32
            ).astype(jnp.bfloat16)
            return carry

        lax.fori_loop(0, (b1 - b0) * (rows // mt), step, 0)

    def give(t, b, cond):
        send(cond, lambda: rc(Pb.at[t, b], R.at[t, b - 2], ps.at[t, b - 2], pr.at[t, b - 2], (ey, f)))

    own_cols = out.shape[1]

    def finish(t, b, cond):
        def fn():
            arrived(R.at[t, b], pr.at[t, b])

            def step(i, carry):
                sl = pl.ds(pl.multiple_of(i * 128, 128), 128)
                F[t, b, sl, :] = (
                    Pb[t, b, sl, :].astype(jnp.float32) + R[t, b, sl, :].astype(jnp.float32)
                ).astype(jnp.bfloat16)
                return carry

            lax.fori_loop(0, rows // 128, step, 0)

        when(cond, fn)
        core = t // (nz // 2)
        idx = lax.rem(t, nz // 2)
        at = (t * 4 + f * 2 + x) * cols - core * own_cols
        dst = out.at[:, pl.ds(pl.multiple_of(at, cols), cols)]
        if b == 1:
            send(cond, lambda: rc(F.at[t, 1], dst, os_.at[t, 0], orr.at[idx, 1 + f], (ex, core)))
            return
        send(cond & (core != f), lambda: rc(F.at[t, 0], dst, os_.at[t, 1], orr.at[idx, 0], sib))

        def keep():
            out[:, pl.ds(pl.multiple_of(at, cols), cols)] = F[t, 0]

        when(cond & (core == f), keep)

    def strips(s):
        if s == 0:
            return [(z, z >= 0)]
        return [(lax.max(z - s, 0), z - s >= 0), (lax.min(z + s, nz - 1), z + s < nz)]

    when(native, lambda: w_load.wait())
    when(native, lambda: own_load.wait())
    when(foreign, lambda: arrived(X.at[0], xr.at[0, 0]))
    normalize(0)
    matmul(z, 0, 1)
    relay(1, 0, native)
    land(2, 1, native)
    relay(0, 1, foreign)
    land(2, 1, foreign)
    rest(2)
    normalize(2)
    near = strips(0) + strips(1)

    def offer(group, b, who):
        for t, c in group:
            when(who & c, lambda t=t: matmul(t, b, b + 1))
            give(t, b, who & c)

    offer(near, 2, True)
    own_x(3)
    relay(1, 1, native)
    offer(strips(2), 2, native)
    zrecv(1, 0, foreign)
    for h, q in flow[:AHEAD]:
        cut_start(h, q)
    land(3, 0, True)
    land(3, 1, True)
    rest(3)
    normalize(3)
    offer(near, 3, True)
    offer(strips(2), 3, native)
    for t, c in near[1:]:
        when(c, lambda t=t: matmul(t, 0, 1))
    land(1, 1, foreign)
    rest(1)
    normalize(1)
    for t, c in near:
        when(c, lambda t=t: matmul(t, 1, 2))
    zrecv(1, 1, foreign)
    offer(strips(2), 3, foreign)
    offer(strips(2), 2, foreign)
    for t, c in strips(2):
        when(c, lambda t=t: matmul(t, 0, 2))
    for i in range(AHEAD, AHEAD + 2):
        cut_sent(*flow[i - AHEAD])
        cut_start(*flow[i])
    for t, c in near:
        finish(t, 0, c)
        finish(t, 1, c)
    for i in range(AHEAD + 2, len(flow)):
        cut_sent(*flow[i - AHEAD])
        cut_start(*flow[i])
    for h, q in flow[-AHEAD:]:
        for c, make in cut(h, q):
            pending.append((foreign & c, make))
    for t, c in strips(2):
        finish(t, 1, c)
        finish(t, 0, c)

    far = nz - 1 - z
    end = (z == 0) | (z == nz - 1)
    core = far // (nz // 2)
    idx = lax.rem(far, nz // 2)
    at = (far * 4 + f * 2 + x) * cols - core * own_cols
    np_ = rows // mt

    def piece(b, u, h):
        sl = pl.ds(u * mt, mt)
        kl = pl.ds(depth - kcut, kcut)

        def fn():
            Pb[far, b, sl, wk(h)] = (A[pl.ds(b * rows + u * mt, mt), :] + jnp.dot(
                Xn[b, sl, kl], Wb[far, kl, wk(h)], preferred_element_type=jnp.float32
            )).astype(jnp.bfloat16)

        when(end, fn)

    def gather(h):
        def step(q, carry):
            kq = pl.ds(pl.multiple_of(q * kcut, kcut), kcut)
            arrived(Wb.at[far, kq, wk(h)], wq.at[1, h, q])
            left = Xn[:, :, kq].reshape(4 * rows, kcut)
            A[...] += jnp.dot(left, Wb[far, kq, wk(h)], preferred_element_type=jnp.float32)
            return carry

        def fn():
            A[...] = jnp.zeros_like(A)
            lax.fori_loop(0, CUTS - 1, step, 0)
            arrived(Wb.at[far, pl.ds(depth - kcut, kcut), wk(h)], wq.at[1, h, CUTS - 1])

        when(end, fn)

    def pass_on(b, u, h, who):
        sl = pl.ds(u * mt, mt)
        k = (b - 2) * np_ + u
        send(end & who, lambda: rc(
            Pb.at[far, b, sl, wk(h)], R.at[far, b - 2, sl, wk(h)],
            psl.at[h, k], prl.at[h, k], (ey, f)))

    def direct(i, b, u, who, dev):
        sl = pl.ds(u * mt, mt)
        send(end & who, lambda: rc(
            Pb.at[far, b, sl, wk(1)], E.at[i, sl], es.at[i, u], er.at[i, u], dev))

    def settle(b, u, h, who):
        sl = pl.ds(u * mt, mt)
        k = b * np_ + u

        def fn():
            arrived(R.at[far, b, sl, wk(h)], prl.at[h, k])
            F[far, b, sl, wk(h)] = (
                Pb[far, b, sl, wk(h)].astype(jnp.float32) + R[far, b, sl, wk(h)].astype(jnp.float32)
            ).astype(jnp.bfloat16)

        when(end & who, fn)
        dst = out.at[sl, pl.ds(pl.multiple_of(at + h * half, half), half)]
        src = F.at[far, b, sl, wk(h)]
        if b == 1:
            send(end & who & who, lambda: rc(src, dst, osl.at[h, k], orr.at[idx, 1 + f], (ex, core)))
        else:
            send(end & who & (core != f), lambda: rc(src, dst, osl.at[h, k], orr.at[idx, 0], sib))

            def keep():
                out[sl, pl.ds(pl.multiple_of(at + h * half, half), half)] = F[far, b, sl, wk(h)]

            when(end & who & (core == f), keep)

    units = range(np_)
    sent = len(pending)
    gather(0)
    for b in (3, 2, 1, 0):
        for u in units:
            piece(b, u, 0)
            if b >= 2:
                pass_on(b, u, 0, True)
    for b in (1, 0):
        for u in units:
            settle(b, u, 0, foreign)
    for cond, make in pending[:sent]:
        when(cond, lambda make=make: make().wait_send())
    del pending[:sent]
    gather(1)
    for u in units:
        piece(2, u, 1)
        pass_on(2, u, 1, True)
    for u in units:
        piece(3, u, 1)
        pass_on(3, u, 1, native)
        direct(1, 3, u, foreign, (ex + ey - env, core))
    for u in units:
        piece(1, u, 1)
        direct(0, 1, u, native, (ex, core))
        settle(1, u, 1, foreign)
    for u in units:
        piece(0, u, 1)
    for b in (1, 0):
        for u in units:
            settle(b, u, 0, native)
    for u in units:
        settle(0, u, 1, True)
    spot = (far * 4 + y * 2 + 1 - x) * cols + half - core * own_cols
    for u in units:
        def join(u=u):
            sl = pl.ds(u * mt, mt)
            for i in range(2):
                arrived(E.at[i, sl], er.at[i, u])
            out[sl, pl.ds(pl.multiple_of(spot, half), half)] = (
                E[0, sl, :].astype(jnp.float32) + E[1, sl, :].astype(jnp.float32)
            ).astype(jnp.bfloat16)

        when(end & (core == f), join)

    for i in range(nz // 2):
        t = f * (nz // 2) + i
        for src in range(3):
            sf = 1 - f if src == 0 else src - 1
            sx = x if src == 0 else 1 - x
            at = (t * 4 + sf * 2 + sx) * cols - f * own_cols
            halved = end & (t == far) & (y == sf) if src else False
            if src:
                when(halved, lambda at=at, i=i, src=src: arrived(
                    out.at[:, pl.ds(pl.multiple_of(at, half), half)], orr.at[i, src]))
            when(jnp.logical_not(halved) if src else True, lambda at=at, i=i, src=src: arrived(
                out.at[:, pl.ds(pl.multiple_of(at, cols), cols)], orr.at[i, src]))
    for cond, make in pending:
        when(cond, lambda make=make: make().wait_send())


def write_back(pieces, mean, var, logits, mean_out, var_out, out, sems):
    size = out.shape[0] // pieces
    copies = [
        pltpu.make_async_copy(logits.at[pl.ds(i * size, size)], out.at[pl.ds(i * size, size)], sems.at[i])
        for i in range(pieces)
    ]
    copies.append(pltpu.make_async_copy(mean, mean_out, sems.at[pieces]))
    copies.append(pltpu.make_async_copy(var, var_out, sems.at[pieces + 1]))
    for copy in copies:
        copy.start()
    for copy in copies:
        copy.wait()


def f_of_y(y):
    return y


def shards_planes(nz, observations, prior_count, prior_mean, prior_var, policy_weight):
    rows, depth = observations.shape
    cols = policy_weight.shape[1]
    n = lax.axis_size("env")
    own_cols = cols * n // 2
    bf, f32 = jnp.bfloat16, jnp.float32
    dma = pltpu.SemaphoreType.DMA
    vmem = pl.BlockSpec(memory_space=pltpu.VMEM)
    hbm = pl.BlockSpec(memory_space=pl.ANY)
    scratch = [
        pltpu.VMEM((4, rows, depth), bf),
        pltpu.VMEM((4, rows, depth), bf),
        pltpu.VMEM((nz, depth, cols), bf),
        pltpu.VMEM((nz, 4, rows, cols), bf),
        pltpu.VMEM((nz, 2, rows, cols), bf),
        pltpu.VMEM((nz, 2, rows, cols), bf),
        pltpu.VMEM((4 * rows, cols // 2), f32),
        pltpu.VMEM((2, rows, cols // 2), bf),
        pltpu.VMEM((1, depth), jnp.int32),
        pltpu.VMEM((1, depth), f32),
        pltpu.VMEM((1, depth), f32),
        pltpu.VMEM((2, depth), f32),
        pltpu.VMEM((2, depth), f32),
        pltpu.VMEM((2, depth), f32),
        pltpu.VMEM((2, depth), f32),
        pltpu.VMEM((nz, 2, depth), f32),
        pltpu.VMEM((2, depth), f32),
        pltpu.VMEM((2, depth), f32),
        dma((2,)),
        dma((3,)),
        dma,
        dma((2, rows // 256)),
        dma((2, rows // 256)),
        dma((4,)),
        dma((4, 4)),
        dma,
        dma((4,)),
        dma((2,)),
        dma((2,)),
        dma((2,)),
        dma((2,)),
        dma((2, nz - 2, 2)),
        dma((nz, 2)),
        dma((2, 2, CUTS)),
        dma((2,)),
        dma((nz + 1,)),
        dma((nz + 2,)),
        dma,
        dma,
        dma((nz, 2)),
        dma((nz, 2)),
        dma((nz, 2)),
        dma((nz // 2, 3)),
        dma((2, rows // 128)),
        dma((2, rows // 128)),
        dma((2, rows // 128)),
    ]
    row = lambda a: a.reshape(1, depth)
    run_mean, run_var, logits = pl.pallas_call(
        functools.partial(kernel, nz),
        out_shape=(
            pltpu.VMEM((1, depth), f32),
            pltpu.VMEM((1, depth), f32),
            pltpu.VMEM((rows, own_cols), bf),
        ),
        in_specs=[hbm] * 5,
        out_specs=(vmem, vmem, vmem),
        scratch_shapes=scratch,
        compiler_params=pltpu.CompilerParams(
            collective_id=0, has_side_effects=True, vmem_limit_bytes=58 * 1024 * 1024
        ),
    )(observations, row(prior_count), row(prior_mean), row(prior_var), policy_weight)
    pieces = 4
    run_mean, run_var, logits = pl.pallas_call(
        functools.partial(write_back, pieces),
        out_shape=(
            jax.ShapeDtypeStruct((1, depth), f32),
            jax.ShapeDtypeStruct((1, depth), f32),
            jax.ShapeDtypeStruct((rows, own_cols), bf),
        ),
        in_specs=[vmem] * 3,
        out_specs=(hbm,) * 3,
        scratch_shapes=[dma((pieces + 2,))],
    )(*(pltpu.with_memory_space_constraint(a, pltpu.VMEM) for a in (run_mean, run_var, logits)))
    return run_mean.reshape(depth), run_var.reshape(depth), logits


def plane_count(mesh):
    devices = mesh.devices
    if devices.ndim != 2 or devices.shape[1] != 2 or devices.shape[0] % 8:
        return 0
    base = devices[0, 0].coords
    for i in range(devices.shape[0]):
        for j in range(2):
            at = [a - b for a, b in zip(devices[i, j].coords, base)]
            if at != [i % 2, i // 2 % 2, i // 4]:
                return 0
    return devices.shape[0] // 4


def solution(mesh):
    placed = (P("env", "feat"), P("feat"), P("feat"), P("feat"), P("feat", "env"))
    nz = plane_count(mesh)
    body = functools.partial(shards_planes, nz) if nz == 4 else shards_general
    return jax.shard_map(
        body,
        mesh=mesh,
        in_specs=placed,
        out_specs=(P("feat"), P("feat"), P("env", "feat")),
        check_vma=False,
    )
```

```python
import functools
import jax
import jax.numpy as jnp
from jax import lax
from jax.experimental import pallas as pl
from jax.experimental.pallas import tpu as pltpu
from jax.sharding import PartitionSpec as P

MESH = pl.DeviceIdType.MESH
CUTS = 4
AHEAD = 2


def shards_general(observations, prior_count, prior_mean, prior_var, policy_weight):
    rows = observations.shape[0]
    values = observations.astype(jnp.float32)
    batch_n = jnp.float32(rows * lax.axis_size("env"))
    local_mean = jnp.mean(values, axis=0)
    local_sq = jnp.sum((values - local_mean) ** 2, axis=0)
    batch_mean = lax.psum(jnp.sum(values, axis=0), "env") / batch_n
    shifted = local_sq + float(rows) * (local_mean - batch_mean) ** 2
    batch_m2 = lax.psum(shifted, "env")
    count = prior_count.astype(jnp.float32)
    total = count + batch_n
    delta = batch_mean - prior_mean
    run_mean = prior_mean + delta * batch_n / total
    run_var = (prior_var * count + batch_m2 + delta * delta * count * batch_n / total) / total
    normalized = jnp.clip((values - run_mean) / jnp.sqrt(run_var + 1e-05), -5.0, 5.0).astype(
        jnp.bfloat16
    )
    partial_block = jnp.dot(
        normalized,
        lax.all_gather(policy_weight, "env", axis=1, tiled=True),
        preferred_element_type=jnp.float32,
    ).astype(jnp.bfloat16)
    summed = lax.psum_scatter(partial_block, "feat", scatter_dimension=1, tiled=True)
    return (run_mean, run_var, summed)


def kernel(
    nz, obs, cnt_in, pmean_in, pvar_in, w, mean_out, var_out, out,
    X, Xn, Wb, Pb, R, F, A, E, cnt, pmean, pvar, S0, RX, S1, RY, RZ, NS, NP,
    loc, ploc, vs, vr, wloc, es, er, xs, xr, ds, ys, x3, d3, d1, d2, ws, wr, wq, wys, ss, sr, nsnd, nrcv, ps, pr, os_, orr, psl, prl, osl,
):
    rows, depth = obs.shape
    cols = w.shape[1]
    quarter = rows // 4
    half = cols // 2
    nblk = nz * 4
    env = lax.axis_index("env")
    f = lax.axis_index("feat")
    x = lax.rem(env, 2)
    y = lax.rem(env // 2, 2)
    z = env // 4
    ex = env + 1 - 2 * x
    ey = env + 2 - 4 * y
    sib = (env, 1 - f)
    native = f == y
    foreign = f != y
    pending = []

    def when(cond, fn):
        if cond is True:
            fn()
        else:
            pl.when(cond)(fn)

    def send(cond, make):
        when(cond, lambda: make().start())
        pending.append((cond, make))

    def rc(src, dst, s, r, dev):
        return pltpu.make_async_remote_copy(
            src_ref=src, dst_ref=dst, send_sem=s, recv_sem=r, device_id=dev, device_id_type=MESH
        )

    def arrived(dst, sem):
        pltpu.make_async_copy(dst, dst, sem).wait()

    def rq(ch):
        return pl.ds(ch * quarter, quarter)

    barrier = pltpu.get_barrier_semaphore()

    def greet(dev):
        pl.semaphore_signal(barrier, inc=1, device_id=dev, device_id_type=MESH)

    greet(sib)
    for g in range(2):
        greet((ex, g))
        greet((ey, g))
    for s in range(1, nz):
        greet((lax.rem(env + 4 * s, nblk), f))

    stat_load = pltpu.make_async_copy(obs, Xn.at[0], loc.at[0])
    stat_load.start()
    w_load = pltpu.make_async_copy(w, Wb.at[z], wloc)
    when(native, lambda: w_load.start())
    own_load = pltpu.make_async_copy(obs, X.at[0], loc.at[1])
    when(native, lambda: own_load.start())

    prior = [
        pltpu.make_async_copy(src, dst, ploc.at[i])
        for i, (src, dst) in enumerate(((cnt_in, cnt), (pmean_in, pmean), (pvar_in, pvar)))
    ]
    for copy in prior:
        when(native, lambda copy=copy: copy.start())
    pl.semaphore_wait(barrier, 5 + nz - 1)

    def wk(h):
        return pl.ds(h * half, half)

    def own_w(h):
        send(foreign, lambda: rc(
            w.at[:, wk(h)], Wb.at[z, :, wk(h)], wys.at[h], wr.at[z, h], (ey, f_of_y(y))))

    own_w(0)

    def own_x(ch):
        dst_core = y if ch < 2 else 1 - y
        send(native, lambda: rc(obs.at[rq(ch)], X.at[1, rq(ch)], xs.at[ch], xr.at[1, ch], (ex, dst_core)))

    def own_y(ch):
        dst_core = 1 - y if ch < 2 else y
        send(foreign, lambda: rc(obs.at[rq(ch)], X.at[2, rq(ch)], ys.at[ch], xr.at[2, ch], (ey, dst_core)))

    zup = z + 1 < nz
    zdn = z >= 1
    for h in range(2):
        when(native & zup, lambda h=h: rc(
            w.at[:, wk(h)], Wb.at[z, :, wk(h)], ws.at[0, 0, h], wr.at[z, h], (env + 4, f)).start())
        when(native & zdn, lambda h=h: rc(
            w.at[:, wk(h)], Wb.at[z, :, wk(h)], ws.at[1, 0, h], wr.at[z, h], (env - 4, f)).start())
    own_x(0)

    kcut = depth // CUTS

    def cut(h, q):
        kq = pl.ds(q * kcut, kcut)
        far_s = nz - 2

        def part(t, dev):
            return rc(Wb.at[t, kq, wk(h)], Wb.at[t, kq, wk(h)], wq.at[0, h, q], wq.at[1, h, q], dev)

        return (
            ((z - far_s >= 0) & (z + 1 < nz), lambda: part(z - far_s, (env + 4, f))),
            ((z + far_s < nz) & (z >= 1), lambda: part(z + far_s, (env - 4, f))),
        )

    def cut_start(h, q):
        for c, make in cut(h, q):
            when(foreign & c, lambda make=make: make().start())

    def cut_sent(h, q):
        for c, make in cut(h, q):
            when(foreign & c, lambda make=make: make().wait_send())

    flow = [(h, q) for h in range(2) for q in range(CUTS)]

    def zsend(s, h, who):
        up = who & (z - s >= 0) & (z + 1 < nz)
        down = who & (z + s < nz) & (z >= 1)
        if s == nz - 2:
            for q in range(CUTS):
                for c, make in cut(h, q):
                    send(who & c, make)
            return
        send(up, lambda: rc(
            Wb.at[z - s, :, wk(h)], Wb.at[z - s, :, wk(h)], ws.at[0, s, h], wr.at[z - s, h], (env + 4, f)))
        send(down, lambda: rc(
            Wb.at[z + s, :, wk(h)], Wb.at[z + s, :, wk(h)], ws.at[1, s, h], wr.at[z + s, h], (env - 4, f)))

    def zrecv(s, h, who=True):
        when(who & (z - 1 - s >= 0), lambda: arrived(Wb.at[z - 1 - s, :, wk(h)], wr.at[z - 1 - s, h]))
        when(who & (z + 1 + s < nz), lambda: arrived(Wb.at[z + 1 + s, :, wk(h)], wr.at[z + 1 + s, h]))

    stat_load.wait()
    tile = 512
    strip = 32

    def moments(c, carry):
        cs = pl.ds(pl.multiple_of(c * tile, tile), tile)

        def add(i, acc):
            v = Xn[0, pl.ds(pl.multiple_of(i * strip, strip), strip), cs].astype(jnp.float32)
            return acc + v.reshape(strip // 8, 8, tile).sum(0)

        tot = lax.fori_loop(0, rows // strip, add, jnp.zeros((8, tile), jnp.float32))
        mean = jnp.sum(tot, axis=0, keepdims=True) * (1.0 / rows)

        def add2(i, acc):
            v = Xn[0, pl.ds(pl.multiple_of(i * strip, strip), strip), cs].astype(jnp.float32) - mean
            return acc + (v * v).reshape(strip // 8, 8, tile).sum(0)

        tot2 = lax.fori_loop(0, rows // strip, add2, jnp.zeros((8, tile), jnp.float32))
        S0[0:1, cs] = mean
        S0[1:2, cs] = jnp.sum(tot2, axis=0, keepdims=True)
        return carry

    lax.fori_loop(0, depth // tile, moments, 0)
    send(True, lambda: rc(S0, RX, ss.at[0], sr.at[0], (ex, f)))
    for ch in (2, 1):
        own_x(ch)
    arrived(RX, sr.at[0])
    m0, m1 = S0[0:1, :], RX[0:1, :]
    S1[0:1, :] = 0.5 * (m0 + m1)
    S1[1:2, :] = S0[1:2, :] + RX[1:2, :] + (0.5 * rows) * (m0 - m1) * (m0 - m1)
    send(foreign, lambda: rc(S1, RY, ss.at[1], sr.at[1], (ey, f)))
    own_w(1)
    for ch in (0, 2, 1, 3):
        own_y(ch)
    send(native, lambda: rc(obs, X.at[0], ds, xr.at[0, 0], sib))

    def base(h):
        def fn():
            arrived(Wb.at[z, :, wk(h)], wr.at[z, h])

            @pl.when(zup)
            def _():
                rc(Wb.at[z, :, wk(h)], Wb.at[z, :, wk(h)], ws.at[0, 0, h], wr.at[z, h], (env + 4, f)).start()

            @pl.when(zdn)
            def _():
                rc(Wb.at[z, :, wk(h)], Wb.at[z, :, wk(h)], ws.at[1, 0, h], wr.at[z, h], (env - 4, f)).start()

        when(foreign, fn)
        pending.append((zup, lambda: rc(
            Wb.at[z, :, wk(h)], Wb.at[z, :, wk(h)], ws.at[0, 0, h], wr.at[z, h], (env + 4, f))))
        pending.append((zdn, lambda: rc(
            Wb.at[z, :, wk(h)], Wb.at[z, :, wk(h)], ws.at[1, 0, h], wr.at[z, h], (env - 4, f))))

    base(0)

    @pl.when(native)
    def _():
        arrived(RY, sr.at[1])
        m0, m1 = S1[0:1, :], RY[0:1, :]
        RZ[z, 0:1, :] = 0.5 * (m0 + m1)
        RZ[z, 1:2, :] = S1[1:2, :] + RY[1:2, :] + (1.0 * rows) * (m0 - m1) * (m0 - m1)

    for s in range(1, nz):
        send(native, lambda s=s: rc(
            RZ.at[z], RZ.at[z], ss.at[1 + s], sr.at[2 + z], (lax.rem(env + 4 * s, nblk), f)))
    base(1)

    lb = jnp.where(native, 0, 2)

    def land(b, i, who):
        ch = lb + i
        sl = pl.ds(pl.multiple_of(ch * quarter, quarter), quarter)
        when(who, lambda: arrived(X.at[b, sl], xr.at[b, ch]))
        sem = {1: d1, 2: d2, 3: d3}[b]
        if b == 2:
            send(who, lambda: rc(X.at[2, sl], X.at[3, sl], x3.at[i], xr.at[3, ch], (ex, f)))
        send(who, lambda: rc(X.at[b, sl], X.at[b, sl], sem.at[i], xr.at[b, ch], sib))

    def relay(s, h, who):
        zrecv(s, h, who)
        if s + 1 < nz - 1:
            zsend(s + 1, h, who)

    relay(0, 0, native)
    relay(0, 1, native)
    land(2, 0, native)
    land(1, 0, native)
    land(1, 1, native)
    land(1, 0, foreign)
    relay(0, 0, foreign)
    land(2, 0, foreign)

    @pl.when(native)
    def _():
        for s in range(1, nz):
            o = lax.rem(z + s, nz)
            arrived(RZ.at[o], sr.at[2 + o])
        bmean = RZ[0, 0:1, :]
        for o in range(1, nz):
            bmean = bmean + RZ[o, 0:1, :]
        bmean = bmean * (1.0 / nz)
        m2 = jnp.zeros_like(bmean)
        per = float(rows * 4)
        for o in range(nz):
            dev = RZ[o, 0:1, :] - bmean
            m2 = m2 + RZ[o, 1:2, :] + per * dev * dev
        batch_n = float(rows * nblk)
        for copy in prior:
            copy.wait()
        count = cnt[...].astype(jnp.float32)
        total = count + batch_n
        delta = bmean - pmean[...]
        new_mean = pmean[...] + delta * batch_n / total
        new_var = (pvar[...] * count + m2 + delta * delta * count * batch_n / total) / total
        mean_out[...] = new_mean
        var_out[...] = new_var
        NS[0:1, :] = new_mean
        NS[1:2, :] = 1.0 / jnp.sqrt(new_var + 1e-05)
        NP[...] = NS[...]

    send(native, lambda: rc(NS, NP, nsnd, nrcv, sib))
    for i, ref in enumerate((mean_out, var_out)):
        send(native, lambda i=i, ref=ref: rc(ref, ref, vs.at[i], vr.at[i], (ey, f)))
    when(foreign, lambda: arrived(NP, nrcv))

    def normalize(b):
        def step(i, carry):
            c = i // (rows // 32)
            r = lax.rem(i, rows // 32)
            cs = pl.ds(pl.multiple_of(c * 1024, 1024), 1024)
            sl = pl.ds(pl.multiple_of(r * 32, 32), 32)
            v = X[b, sl, cs].astype(jnp.float32)
            v = (v - NP[0:1, cs]) * NP[1:2, cs]
            Xn[b, sl, cs] = jnp.clip(v, -5.0, 5.0).astype(jnp.bfloat16)
            return carry

        lax.fori_loop(0, (rows // 32) * (depth // 1024), step, 0)

    def rest(b):
        for i in range(2):
            ch = 2 - lb + i
            sl = pl.ds(pl.multiple_of(ch * quarter, quarter), quarter)
            arrived(X.at[b, sl], xr.at[b, ch])

    mt = 256

    def matmul(t, b0, b1):
        def step(i, carry):
            b = b0 + i // (rows // mt)
            sl = pl.ds(pl.multiple_of(lax.rem(i, rows // mt) * mt, mt), mt)
            Pb[t, b, sl, :] = jnp.dot(
                Xn[b, sl, :], Wb[t], preferred_element_type=jnp.float32
            ).astype(jnp.bfloat16)
            return carry

        lax.fori_loop(0, (b1 - b0) * (rows // mt), step, 0)

    def give(t, b, cond):
        send(cond, lambda: rc(Pb.at[t, b], R.at[t, b - 2], ps.at[t, b - 2], pr.at[t, b - 2], (ey, f)))

    own_cols = out.shape[1]

    def finish(t, b, cond):
        def fn():
            arrived(R.at[t, b], pr.at[t, b])

            def step(i, carry):
                sl = pl.ds(pl.multiple_of(i * 128, 128), 128)
                F[t, b, sl, :] = (
                    Pb[t, b, sl, :].astype(jnp.float32) + R[t, b, sl, :].astype(jnp.float32)
                ).astype(jnp.bfloat16)
                return carry

            lax.fori_loop(0, rows // 128, step, 0)

        when(cond, fn)
        core = t // (nz // 2)
        idx = lax.rem(t, nz // 2)
        at = (t * 4 + f * 2 + x) * cols - core * own_cols
        dst = out.at[:, pl.ds(pl.multiple_of(at, cols), cols)]
        if b == 1:
            send(cond, lambda: rc(F.at[t, 1], dst, os_.at[t, 0], orr.at[idx, 1 + f], (ex, core)))
            return
        send(cond & (core != f), lambda: rc(F.at[t, 0], dst, os_.at[t, 1], orr.at[idx, 0], sib))

        def keep():
            out[:, pl.ds(pl.multiple_of(at, cols), cols)] = F[t, 0]

        when(cond & (core == f), keep)

    def strips(s):
        if s == 0:
            return [(z, z >= 0)]
        return [(lax.max(z - s, 0), z - s >= 0), (lax.min(z + s, nz - 1), z + s < nz)]

    when(native, lambda: w_load.wait())
    when(native, lambda: own_load.wait())
    when(foreign, lambda: arrived(X.at[0], xr.at[0, 0]))
    normalize(0)
    matmul(z, 0, 1)
    relay(1, 0, native)
    land(2, 1, native)
    relay(0, 1, foreign)
    land(2, 1, foreign)
    rest(2)
    normalize(2)
    near = strips(0) + strips(1)

    def offer(group, b, who):
        for t, c in group:
            when(who & c, lambda t=t: matmul(t, b, b + 1))
            give(t, b, who & c)

    offer(near, 2, True)
    own_x(3)
    relay(1, 1, native)
    offer(strips(2), 2, native)
    zrecv(1, 0, foreign)
    for h, q in flow[:AHEAD]:
        cut_start(h, q)
    land(3, 0, True)
    land(3, 1, True)
    rest(3)
    normalize(3)
    offer(near, 3, True)
    offer(strips(2), 3, native)
    for t, c in near[1:]:
        when(c, lambda t=t: matmul(t, 0, 1))
    land(1, 1, foreign)
    rest(1)
    normalize(1)
    for t, c in near:
        when(c, lambda t=t: matmul(t, 1, 2))
    zrecv(1, 1, foreign)
    offer(strips(2), 3, foreign)
    offer(strips(2), 2, foreign)
    for t, c in strips(2):
        when(c, lambda t=t: matmul(t, 0, 2))
    for i in range(AHEAD, AHEAD + 2):
        cut_sent(*flow[i - AHEAD])
        cut_start(*flow[i])
    for t, c in near:
        finish(t, 0, c)
        finish(t, 1, c)
    for i in range(AHEAD + 2, len(flow)):
        cut_sent(*flow[i - AHEAD])
        cut_start(*flow[i])
    for h, q in flow[-AHEAD:]:
        for c, make in cut(h, q):
            pending.append((foreign & c, make))
    for t, c in strips(2):
        finish(t, 1, c)
        finish(t, 0, c)

    far = nz - 1 - z
    end = (z == 0) | (z == nz - 1)
    core = far // (nz // 2)
    idx = lax.rem(far, nz // 2)
    at = (far * 4 + f * 2 + x) * cols - core * own_cols
    np_ = rows // mt

    def piece(b, u, h):
        sl = pl.ds(u * mt, mt)
        kl = pl.ds(depth - kcut, kcut)

        def fn():
            Pb[far, b, sl, wk(h)] = (A[pl.ds(b * rows + u * mt, mt), :] + jnp.dot(
                Xn[b, sl, kl], Wb[far, kl, wk(h)], preferred_element_type=jnp.float32
            )).astype(jnp.bfloat16)

        when(end, fn)

    def gather(h):
        def step(q, carry):
            kq = pl.ds(pl.multiple_of(q * kcut, kcut), kcut)
            arrived(Wb.at[far, kq, wk(h)], wq.at[1, h, q])
            left = Xn[:, :, kq].reshape(4 * rows, kcut)
            A[...] += jnp.dot(left, Wb[far, kq, wk(h)], preferred_element_type=jnp.float32)
            return carry

        def fn():
            A[...] = jnp.zeros_like(A)
            lax.fori_loop(0, CUTS - 1, step, 0)
            arrived(Wb.at[far, pl.ds(depth - kcut, kcut), wk(h)], wq.at[1, h, CUTS - 1])

        when(end, fn)

    def pass_on(b, u, h, who):
        sl = pl.ds(u * mt, mt)
        k = (b - 2) * np_ + u
        send(end & who, lambda: rc(
            Pb.at[far, b, sl, wk(h)], R.at[far, b - 2, sl, wk(h)],
            psl.at[h, k], prl.at[h, k], (ey, f)))

    def direct(i, b, u, who, dev):
        sl = pl.ds(u * mt, mt)
        send(end & who, lambda: rc(
            Pb.at[far, b, sl, wk(1)], E.at[i, sl], es.at[i, u], er.at[i, u], dev))

    def settle(b, u, h, who):
        sl = pl.ds(u * mt, mt)
        k = b * np_ + u

        def fn():
            arrived(R.at[far, b, sl, wk(h)], prl.at[h, k])
            F[far, b, sl, wk(h)] = (
                Pb[far, b, sl, wk(h)].astype(jnp.float32) + R[far, b, sl, wk(h)].astype(jnp.float32)
            ).astype(jnp.bfloat16)

        when(end & who, fn)
        dst = out.at[sl, pl.ds(pl.multiple_of(at + h * half, half), half)]
        src = F.at[far, b, sl, wk(h)]
        if b == 1:
            send(end & who & who, lambda: rc(src, dst, osl.at[h, k], orr.at[idx, 1 + f], (ex, core)))
        else:
            send(end & who & (core != f), lambda: rc(src, dst, osl.at[h, k], orr.at[idx, 0], sib))

            def keep():
                out[sl, pl.ds(pl.multiple_of(at + h * half, half), half)] = F[far, b, sl, wk(h)]

            when(end & who & (core == f), keep)

    units = range(np_)
    sent = len(pending)
    gather(0)
    for b in (3, 2, 1, 0):
        for u in units:
            piece(b, u, 0)
            if b >= 2:
                pass_on(b, u, 0, True)
    for b in (1, 0):
        for u in units:
            settle(b, u, 0, foreign)
    for i, ref in enumerate((mean_out, var_out)):
        when(foreign, lambda i=i, ref=ref: arrived(ref, vr.at[i]))
    for cond, make in pending[:sent]:
        when(cond, lambda make=make: make().wait_send())
    del pending[:sent]
    gather(1)
    for u in units:
        piece(2, u, 1)
        pass_on(2, u, 1, True)
    for u in units:
        piece(3, u, 1)
        pass_on(3, u, 1, native)
        direct(1, 3, u, foreign, (ex + ey - env, core))
    for u in units:
        piece(1, u, 1)
        direct(0, 1, u, native, (ex, core))
        settle(1, u, 1, foreign)
    for u in units:
        piece(0, u, 1)
    for b in (1, 0):
        for u in units:
            settle(b, u, 0, native)
    for u in units:
        settle(0, u, 1, True)
    spot = (far * 4 + y * 2 + 1 - x) * cols + half - core * own_cols
    for u in units:
        def join(u=u):
            sl = pl.ds(u * mt, mt)
            for i in range(2):
                arrived(E.at[i, sl], er.at[i, u])
            out[sl, pl.ds(pl.multiple_of(spot, half), half)] = (
                E[0, sl, :].astype(jnp.float32) + E[1, sl, :].astype(jnp.float32)
            ).astype(jnp.bfloat16)

        when(end & (core == f), join)

    for i in range(nz // 2):
        t = f * (nz // 2) + i
        for src in range(3):
            sf = 1 - f if src == 0 else src - 1
            sx = x if src == 0 else 1 - x
            at = (t * 4 + sf * 2 + sx) * cols - f * own_cols
            halved = end & (t == far) & (y == sf) if src else False
            if src:
                when(halved, lambda at=at, i=i, src=src: arrived(
                    out.at[:, pl.ds(pl.multiple_of(at, half), half)], orr.at[i, src]))
            when(jnp.logical_not(halved) if src else True, lambda at=at, i=i, src=src: arrived(
                out.at[:, pl.ds(pl.multiple_of(at, cols), cols)], orr.at[i, src]))
    for cond, make in pending:
        when(cond, lambda make=make: make().wait_send())


def write_back(pieces, mean, var, logits, mean_out, var_out, out, sems):
    size = out.shape[0] // pieces
    copies = [
        pltpu.make_async_copy(logits.at[pl.ds(i * size, size)], out.at[pl.ds(i * size, size)], sems.at[i])
        for i in range(pieces)
    ]
    copies.append(pltpu.make_async_copy(mean, mean_out, sems.at[pieces]))
    copies.append(pltpu.make_async_copy(var, var_out, sems.at[pieces + 1]))
    for copy in copies:
        copy.start()
    for copy in copies:
        copy.wait()


def f_of_y(y):
    return y


def shards_planes(nz, observations, prior_count, prior_mean, prior_var, policy_weight):
    rows, depth = observations.shape
    cols = policy_weight.shape[1]
    n = lax.axis_size("env")
    own_cols = cols * n // 2
    bf, f32 = jnp.bfloat16, jnp.float32
    dma = pltpu.SemaphoreType.DMA
    vmem = pl.BlockSpec(memory_space=pltpu.VMEM)
    hbm = pl.BlockSpec(memory_space=pl.ANY)
    scratch = [
        pltpu.VMEM((4, rows, depth), bf),
        pltpu.VMEM((4, rows, depth), bf),
        pltpu.VMEM((nz, depth, cols), bf),
        pltpu.VMEM((nz, 4, rows, cols), bf),
        pltpu.VMEM((nz, 2, rows, cols), bf),
        pltpu.VMEM((nz, 2, rows, cols), bf),
        pltpu.VMEM((4 * rows, cols // 2), f32),
        pltpu.VMEM((2, rows, cols // 2), bf),
        pltpu.VMEM((1, depth), jnp.int32),
        pltpu.VMEM((1, depth), f32),
        pltpu.VMEM((1, depth), f32),
        pltpu.VMEM((2, depth), f32),
        pltpu.VMEM((2, depth), f32),
        pltpu.VMEM((2, depth), f32),
        pltpu.VMEM((2, depth), f32),
        pltpu.VMEM((nz, 2, depth), f32),
        pltpu.VMEM((2, depth), f32),
        pltpu.VMEM((2, depth), f32),
        dma((2,)),
        dma((3,)),
        dma((2,)),
        dma((2,)),
        dma,
        dma((2, rows // 256)),
        dma((2, rows // 256)),
        dma((4,)),
        dma((4, 4)),
        dma,
        dma((4,)),
        dma((2,)),
        dma((2,)),
        dma((2,)),
        dma((2,)),
        dma((2, nz - 2, 2)),
        dma((nz, 2)),
        dma((2, 2, CUTS)),
        dma((2,)),
        dma((nz + 1,)),
        dma((nz + 2,)),
        dma,
        dma,
        dma((nz, 2)),
        dma((nz, 2)),
        dma((nz, 2)),
        dma((nz // 2, 3)),
        dma((2, rows // 128)),
        dma((2, rows // 128)),
        dma((2, rows // 128)),
    ]
    row = lambda a: a.reshape(1, depth)
    run_mean, run_var, logits = pl.pallas_call(
        functools.partial(kernel, nz),
        out_shape=(
            pltpu.VMEM((1, depth), f32),
            pltpu.VMEM((1, depth), f32),
            pltpu.VMEM((rows, own_cols), bf),
        ),
        in_specs=[hbm] * 5,
        out_specs=(vmem, vmem, vmem),
        scratch_shapes=scratch,
        compiler_params=pltpu.CompilerParams(
            collective_id=0, has_side_effects=True, vmem_limit_bytes=58 * 1024 * 1024
        ),
    )(observations, row(prior_count), row(prior_mean), row(prior_var), policy_weight)
    pieces = 4
    run_mean, run_var, logits = pl.pallas_call(
        functools.partial(write_back, pieces),
        out_shape=(
            jax.ShapeDtypeStruct((1, depth), f32),
            jax.ShapeDtypeStruct((1, depth), f32),
            jax.ShapeDtypeStruct((rows, own_cols), bf),
        ),
        in_specs=[vmem] * 3,
        out_specs=(hbm,) * 3,
        scratch_shapes=[dma((pieces + 2,))],
    )(*(pltpu.with_memory_space_constraint(a, pltpu.VMEM) for a in (run_mean, run_var, logits)))
    return run_mean.reshape(depth), run_var.reshape(depth), logits


def plane_count(mesh):
    devices = mesh.devices
    if devices.ndim != 2 or devices.shape[1] != 2 or devices.shape[0] % 8:
        return 0
    base = devices[0, 0].coords
    for i in range(devices.shape[0]):
        for j in range(2):
            at = [a - b for a, b in zip(devices[i, j].coords, base)]
            if at != [i % 2, i // 2 % 2, i // 4]:
                return 0
    return devices.shape[0] // 4


def solution(mesh):
    placed = (P("env", "feat"), P("feat"), P("feat"), P("feat"), P("feat", "env"))
    nz = plane_count(mesh)
    body = functools.partial(shards_planes, nz) if nz == 4 else shards_general
    return jax.shard_map(
        body,
        mesh=mesh,
        in_specs=placed,
        out_specs=(P("feat"), P("feat"), P("env", "feat")),
        check_vma=False,
    )
```

```python
import functools
import jax
import jax.numpy as jnp
from jax import lax
from jax.experimental import pallas as pl
from jax.experimental.pallas import tpu as pltpu
from jax.sharding import PartitionSpec as P

MESH = pl.DeviceIdType.MESH
CUTS = 4
AHEAD = 2


def shards_general(observations, prior_count, prior_mean, prior_var, policy_weight):
    rows = observations.shape[0]
    values = observations.astype(jnp.float32)
    batch_n = jnp.float32(rows * lax.axis_size("env"))
    local_mean = jnp.mean(values, axis=0)
    local_sq = jnp.sum((values - local_mean) ** 2, axis=0)
    batch_mean = lax.psum(jnp.sum(values, axis=0), "env") / batch_n
    shifted = local_sq + float(rows) * (local_mean - batch_mean) ** 2
    batch_m2 = lax.psum(shifted, "env")
    count = prior_count.astype(jnp.float32)
    total = count + batch_n
    delta = batch_mean - prior_mean
    run_mean = prior_mean + delta * batch_n / total
    run_var = (prior_var * count + batch_m2 + delta * delta * count * batch_n / total) / total
    normalized = jnp.clip((values - run_mean) / jnp.sqrt(run_var + 1e-05), -5.0, 5.0).astype(
        jnp.bfloat16
    )
    partial_block = jnp.dot(
        normalized,
        lax.all_gather(policy_weight, "env", axis=1, tiled=True),
        preferred_element_type=jnp.float32,
    ).astype(jnp.bfloat16)
    summed = lax.psum_scatter(partial_block, "feat", scatter_dimension=1, tiled=True)
    return (run_mean, run_var, summed)


def kernel(
    nz, obs, cnt_in, pmean_in, pvar_in, w, mean_out, var_out, out,
    X, Xn, Wb, Pb, R, F, A, E, cnt, pmean, pvar, S0, RX, S1, RY, RZ, NS, NP,
    loc, ploc, vs, vr, wloc, es, er, xs, xr, ds, x3, d3, d1, d2, ws, wr, wq, wys, ss, sr, nsnd, nrcv, ps, pr, os_, orr, psl, prl, osl,
):
    rows, depth = obs.shape
    cols = w.shape[1]
    quarter = rows // 4
    half = cols // 2
    nblk = nz * 4
    env = lax.axis_index("env")
    f = lax.axis_index("feat")
    x = lax.rem(env, 2)
    y = lax.rem(env // 2, 2)
    z = env // 4
    ex = env + 1 - 2 * x
    ey = env + 2 - 4 * y
    sib = (env, 1 - f)
    native = f == y
    foreign = f != y
    pending = []

    def when(cond, fn):
        if cond is True:
            fn()
        else:
            pl.when(cond)(fn)

    def send(cond, make):
        when(cond, lambda: make().start())
        pending.append((cond, make))

    def rc(src, dst, s, r, dev):
        return pltpu.make_async_remote_copy(
            src_ref=src, dst_ref=dst, send_sem=s, recv_sem=r, device_id=dev, device_id_type=MESH
        )

    def arrived(dst, sem):
        pltpu.make_async_copy(dst, dst, sem).wait()

    def rq(ch):
        return pl.ds(ch * quarter, quarter)

    barrier = pltpu.get_barrier_semaphore()

    def greet(dev):
        pl.semaphore_signal(barrier, inc=1, device_id=dev, device_id_type=MESH)

    greet(sib)
    for g in range(2):
        greet((ex, g))
        greet((ey, g))
    for s in range(1, nz):
        greet((lax.rem(env + 4 * s, nblk), f))

    def wk(h):
        return pl.ds(h * half, half)

    w_load = [pltpu.make_async_copy(w.at[:, wk(h)], Wb.at[z, :, wk(h)], wloc.at[h]) for h in range(2)]
    for copy in w_load:
        when(native, lambda copy=copy: copy.start())
    stat_load = pltpu.make_async_copy(obs, Xn.at[0], loc.at[0])
    stat_load.start()
    own_load = pltpu.make_async_copy(obs, X.at[0], loc.at[1])
    when(native, lambda: own_load.start())

    prior = [
        pltpu.make_async_copy(src, dst, ploc.at[i])
        for i, (src, dst) in enumerate(((cnt_in, cnt), (pmean_in, pmean), (pvar_in, pvar)))
    ]
    for copy in prior:
        when(native, lambda copy=copy: copy.start())
    pl.semaphore_wait(barrier, 5 + nz - 1)

    def own_w(h):
        send(foreign, lambda: rc(
            w.at[:, wk(h)], Wb.at[z, :, wk(h)], wys.at[h], wr.at[z, h], (ey, f_of_y(y))))

    own_w(0)

    def own_x(ch):
        dst_core = y if ch < 2 else 1 - y
        send(native, lambda: rc(obs.at[rq(ch)], X.at[1, rq(ch)], xs.at[ch], xr.at[1, ch], (ex, dst_core)))

    def own_y(ch):
        dst_core = 1 - y if ch < 2 else y
        send(foreign, lambda: rc(obs.at[rq(ch)], X.at[2, rq(ch)], xs.at[ch], xr.at[2, ch], (ey, dst_core)))

    zup = z + 1 < nz
    zdn = z >= 1
    for h in range(2):
        when(native, lambda h=h: w_load[h].wait())
        when(native & zup, lambda h=h: rc(
            Wb.at[z, :, wk(h)], Wb.at[z, :, wk(h)], ws.at[0, 0, h], wr.at[z, h], (env + 4, f)).start())
        when(native & zdn, lambda h=h: rc(
            Wb.at[z, :, wk(h)], Wb.at[z, :, wk(h)], ws.at[1, 0, h], wr.at[z, h], (env - 4, f)).start())
    own_x(0)

    kcut = depth // CUTS

    def cut(h, q):
        kq = pl.ds(q * kcut, kcut)
        far_s = nz - 2

        def part(t, dev):
            return rc(Wb.at[t, kq, wk(h)], Wb.at[t, kq, wk(h)], wq.at[0, h, q], wq.at[1, h, q], dev)

        return (
            ((z - far_s >= 0) & (z + 1 < nz), lambda: part(z - far_s, (env + 4, f))),
            ((z + far_s < nz) & (z >= 1), lambda: part(z + far_s, (env - 4, f))),
        )

    def cut_start(h, q):
        for c, make in cut(h, q):
            when(foreign & c, lambda make=make: make().start())

    def cut_sent(h, q):
        for c, make in cut(h, q):
            when(foreign & c, lambda make=make: make().wait_send())

    flow = [(h, q) for h in range(2) for q in range(CUTS)]

    def zsend(s, h, who):
        up = who & (z - s >= 0) & (z + 1 < nz)
        down = who & (z + s < nz) & (z >= 1)
        if s == nz - 2:
            for q in range(CUTS):
                for c, make in cut(h, q):
                    send(who & c, make)
            return
        send(up, lambda: rc(
            Wb.at[z - s, :, wk(h)], Wb.at[z - s, :, wk(h)], ws.at[0, s, h], wr.at[z - s, h], (env + 4, f)))
        send(down, lambda: rc(
            Wb.at[z + s, :, wk(h)], Wb.at[z + s, :, wk(h)], ws.at[1, s, h], wr.at[z + s, h], (env - 4, f)))

    def zrecv(s, h, who=True):
        when(who & (z - 1 - s >= 0), lambda: arrived(Wb.at[z - 1 - s, :, wk(h)], wr.at[z - 1 - s, h]))
        when(who & (z + 1 + s < nz), lambda: arrived(Wb.at[z + 1 + s, :, wk(h)], wr.at[z + 1 + s, h]))

    stat_load.wait()
    tile = 512
    strip = 32

    def moments(c, carry):
        cs = pl.ds(pl.multiple_of(c * tile, tile), tile)

        def add(i, acc):
            v = Xn[0, pl.ds(pl.multiple_of(i * strip, strip), strip), cs].astype(jnp.float32)
            return acc + v.reshape(strip // 8, 8, tile).sum(0)

        tot = lax.fori_loop(0, rows // strip, add, jnp.zeros((8, tile), jnp.float32))
        mean = jnp.sum(tot, axis=0, keepdims=True) * (1.0 / rows)

        def add2(i, acc):
            v = Xn[0, pl.ds(pl.multiple_of(i * strip, strip), strip), cs].astype(jnp.float32) - mean
            return acc + (v * v).reshape(strip // 8, 8, tile).sum(0)

        tot2 = lax.fori_loop(0, rows // strip, add2, jnp.zeros((8, tile), jnp.float32))
        S0[0:1, cs] = mean
        S0[1:2, cs] = jnp.sum(tot2, axis=0, keepdims=True)
        return carry

    lax.fori_loop(0, depth // tile, moments, 0)
    send(True, lambda: rc(S0, RX, ss.at[0], sr.at[0], (ex, f)))
    for ch in (2, 1):
        own_x(ch)
    arrived(RX, sr.at[0])
    m0, m1 = S0[0:1, :], RX[0:1, :]
    S1[0:1, :] = 0.5 * (m0 + m1)
    S1[1:2, :] = S0[1:2, :] + RX[1:2, :] + (0.5 * rows) * (m0 - m1) * (m0 - m1)
    send(foreign, lambda: rc(S1, RY, ss.at[1], sr.at[1], (ey, f)))
    own_w(1)
    for ch in (0, 2, 1, 3):
        own_y(ch)
    send(native, lambda: rc(obs, X.at[0], ds, xr.at[0, 0], sib))

    def base(h):
        def fn():
            arrived(Wb.at[z, :, wk(h)], wr.at[z, h])

            @pl.when(zup)
            def _():
                rc(Wb.at[z, :, wk(h)], Wb.at[z, :, wk(h)], ws.at[0, 0, h], wr.at[z, h], (env + 4, f)).start()

            @pl.when(zdn)
            def _():
                rc(Wb.at[z, :, wk(h)], Wb.at[z, :, wk(h)], ws.at[1, 0, h], wr.at[z, h], (env - 4, f)).start()

        when(foreign, fn)
        pending.append((zup, lambda: rc(
            Wb.at[z, :, wk(h)], Wb.at[z, :, wk(h)], ws.at[0, 0, h], wr.at[z, h], (env + 4, f))))
        pending.append((zdn, lambda: rc(
            Wb.at[z, :, wk(h)], Wb.at[z, :, wk(h)], ws.at[1, 0, h], wr.at[z, h], (env - 4, f))))

    base(0)

    @pl.when(native)
    def _():
        arrived(RY, sr.at[1])
        m0, m1 = S1[0:1, :], RY[0:1, :]
        RZ[z, 0:1, :] = 0.5 * (m0 + m1)
        RZ[z, 1:2, :] = S1[1:2, :] + RY[1:2, :] + (1.0 * rows) * (m0 - m1) * (m0 - m1)

    for s in range(1, nz):
        send(native, lambda s=s: rc(
            RZ.at[z], RZ.at[z], ss.at[1 + s], sr.at[2 + z], (lax.rem(env + 4 * s, nblk), f)))
    base(1)

    lb = jnp.where(native, 0, 2)

    def land(b, i, who):
        ch = lb + i
        sl = pl.ds(pl.multiple_of(ch * quarter, quarter), quarter)
        when(who, lambda: arrived(X.at[b, sl], xr.at[b, ch]))
        sem = {1: d1, 2: d2, 3: d3}[b]
        if b == 2:
            send(who, lambda: rc(X.at[2, sl], X.at[3, sl], x3.at[i], xr.at[3, ch], (ex, f)))
        send(who, lambda: rc(X.at[b, sl], X.at[b, sl], sem.at[i], xr.at[b, ch], sib))

    def relay(s, h, who):
        zrecv(s, h, who)
        if s + 1 < nz - 1:
            zsend(s + 1, h, who)

    relay(0, 0, native)
    relay(0, 1, native)
    land(2, 0, native)
    land(1, 0, native)
    land(1, 1, native)
    land(1, 0, foreign)
    relay(0, 0, foreign)
    land(2, 0, foreign)

    @pl.when(native)
    def _():
        for s in range(1, nz):
            o = lax.rem(z + s, nz)
            arrived(RZ.at[o], sr.at[2 + o])
        bmean = RZ[0, 0:1, :]
        for o in range(1, nz):
            bmean = bmean + RZ[o, 0:1, :]
        bmean = bmean * (1.0 / nz)
        m2 = jnp.zeros_like(bmean)
        per = float(rows * 4)
        for o in range(nz):
            dev = RZ[o, 0:1, :] - bmean
            m2 = m2 + RZ[o, 1:2, :] + per * dev * dev
        batch_n = float(rows * nblk)
        for copy in prior:
            copy.wait()
        count = cnt[...].astype(jnp.float32)
        total = count + batch_n
        delta = bmean - pmean[...]
        new_mean = pmean[...] + delta * batch_n / total
        new_var = (pvar[...] * count + m2 + delta * delta * count * batch_n / total) / total
        mean_out[...] = new_mean
        var_out[...] = new_var
        NS[0:1, :] = new_mean
        NS[1:2, :] = 1.0 / jnp.sqrt(new_var + 1e-05)
        NP[...] = NS[...]

    send(native, lambda: rc(NS, NP, nsnd, nrcv, sib))
    for i, ref in enumerate((mean_out, var_out)):
        send(native, lambda i=i, ref=ref: rc(ref, ref, vs.at[i], vr.at[i], (ey, f)))
    when(foreign, lambda: arrived(NP, nrcv))

    def normalize(b):
        def step(i, carry):
            c = i // (rows // 32)
            r = lax.rem(i, rows // 32)
            cs = pl.ds(pl.multiple_of(c * 1024, 1024), 1024)
            sl = pl.ds(pl.multiple_of(r * 32, 32), 32)
            v = X[b, sl, cs].astype(jnp.float32)
            v = (v - NP[0:1, cs]) * NP[1:2, cs]
            Xn[b, sl, cs] = jnp.clip(v, -5.0, 5.0).astype(jnp.bfloat16)
            return carry

        lax.fori_loop(0, (rows // 32) * (depth // 1024), step, 0)

    def rest(b):
        for i in range(2):
            ch = 2 - lb + i
            sl = pl.ds(pl.multiple_of(ch * quarter, quarter), quarter)
            arrived(X.at[b, sl], xr.at[b, ch])

    mt = 256

    def matmul(t, b0, b1):
        def step(i, carry):
            b = b0 + i // (rows // mt)
            sl = pl.ds(pl.multiple_of(lax.rem(i, rows // mt) * mt, mt), mt)
            Pb[t, b, sl, :] = jnp.dot(
                Xn[b, sl, :], Wb[t], preferred_element_type=jnp.float32
            ).astype(jnp.bfloat16)
            return carry

        lax.fori_loop(0, (b1 - b0) * (rows // mt), step, 0)

    def give(t, b, cond):
        send(cond, lambda: rc(Pb.at[t, b], R.at[t, b - 2], ps.at[t, b - 2], pr.at[t, b - 2], (ey, f)))

    own_cols = out.shape[1]

    def finish(t, b, cond):
        def fn():
            arrived(R.at[t, b], pr.at[t, b])

            def step(i, carry):
                sl = pl.ds(pl.multiple_of(i * 128, 128), 128)
                F[t, b, sl, :] = (
                    Pb[t, b, sl, :].astype(jnp.float32) + R[t, b, sl, :].astype(jnp.float32)
                ).astype(jnp.bfloat16)
                return carry

            lax.fori_loop(0, rows // 128, step, 0)

        when(cond, fn)
        core = t // (nz // 2)
        idx = lax.rem(t, nz // 2)
        at = (t * 4 + f * 2 + x) * cols - core * own_cols
        dst = out.at[:, pl.ds(pl.multiple_of(at, cols), cols)]
        if b == 1:
            send(cond, lambda: rc(F.at[t, 1], dst, os_.at[t, 0], orr.at[idx, 1 + f], (ex, core)))
            return
        send(cond & (core != f), lambda: rc(F.at[t, 0], dst, os_.at[t, 1], orr.at[idx, 0], sib))

        def keep():
            out[:, pl.ds(pl.multiple_of(at, cols), cols)] = F[t, 0]

        when(cond & (core == f), keep)

    def strips(s):
        if s == 0:
            return [(z, z >= 0)]
        return [(lax.max(z - s, 0), z - s >= 0), (lax.min(z + s, nz - 1), z + s < nz)]

    when(native, lambda: own_load.wait())
    when(foreign, lambda: arrived(X.at[0], xr.at[0, 0]))
    normalize(0)
    matmul(z, 0, 1)
    relay(1, 0, native)
    land(2, 1, native)
    relay(0, 1, foreign)
    land(2, 1, foreign)
    rest(2)
    normalize(2)
    near = strips(0) + strips(1)

    def offer(group, b, who):
        for t, c in group:
            when(who & c, lambda t=t: matmul(t, b, b + 1))
            give(t, b, who & c)

    offer(near, 2, True)
    own_x(3)
    relay(1, 1, native)
    offer(strips(2), 2, native)
    zrecv(1, 0, foreign)
    for h, q in flow[:AHEAD]:
        cut_start(h, q)
    land(3, 0, True)
    land(3, 1, True)
    rest(3)
    normalize(3)
    offer(near, 3, True)
    offer(strips(2), 3, native)
    for t, c in near[1:]:
        when(c, lambda t=t: matmul(t, 0, 1))
    land(1, 1, foreign)
    rest(1)
    normalize(1)
    for t, c in near:
        when(c, lambda t=t: matmul(t, 1, 2))
    zrecv(1, 1, foreign)
    offer(strips(2), 3, foreign)
    offer(strips(2), 2, foreign)
    for t, c in strips(2):
        when(c, lambda t=t: matmul(t, 0, 2))
    for i in range(AHEAD, AHEAD + 2):
        cut_sent(*flow[i - AHEAD])
        cut_start(*flow[i])
    for t, c in near:
        finish(t, 0, c)
        finish(t, 1, c)
    for i in range(AHEAD + 2, len(flow)):
        cut_sent(*flow[i - AHEAD])
        cut_start(*flow[i])
    for h, q in flow[-AHEAD:]:
        for c, make in cut(h, q):
            pending.append((foreign & c, make))
    for t, c in strips(2):
        finish(t, 1, c)
        finish(t, 0, c)

    far = nz - 1 - z
    end = (z == 0) | (z == nz - 1)
    core = far // (nz // 2)
    idx = lax.rem(far, nz // 2)
    at = (far * 4 + f * 2 + x) * cols - core * own_cols
    np_ = rows // mt

    def piece(b, u, h):
        sl = pl.ds(u * mt, mt)
        kl = pl.ds(depth - kcut, kcut)

        def fn():
            Pb[far, b, sl, wk(h)] = (A[pl.ds(b * rows + u * mt, mt), :] + jnp.dot(
                Xn[b, sl, kl], Wb[far, kl, wk(h)], preferred_element_type=jnp.float32
            )).astype(jnp.bfloat16)

        when(end, fn)

    def gather(h):
        def step(q, carry):
            kq = pl.ds(pl.multiple_of(q * kcut, kcut), kcut)
            arrived(Wb.at[far, kq, wk(h)], wq.at[1, h, q])
            left = Xn[:, :, kq].reshape(4 * rows, kcut)
            A[...] += jnp.dot(left, Wb[far, kq, wk(h)], preferred_element_type=jnp.float32)
            return carry

        def fn():
            A[...] = jnp.zeros_like(A)
            lax.fori_loop(0, CUTS - 1, step, 0)
            arrived(Wb.at[far, pl.ds(depth - kcut, kcut), wk(h)], wq.at[1, h, CUTS - 1])

        when(end, fn)

    def pass_on(b, u, h, who):
        sl = pl.ds(u * mt, mt)
        k = (b - 2) * np_ + u
        send(end & who, lambda: rc(
            Pb.at[far, b, sl, wk(h)], R.at[far, b - 2, sl, wk(h)],
            psl.at[h, k], prl.at[h, k], (ey, f)))

    def direct(i, b, u, who, dev):
        sl = pl.ds(u * mt, mt)
        send(end & who, lambda: rc(
            Pb.at[far, b, sl, wk(1)], E.at[i, sl], es.at[u], er.at[i, u], dev))

    def settle(b, u, h, who):
        sl = pl.ds(u * mt, mt)
        k = b * np_ + u

        def fn():
            arrived(R.at[far, b, sl, wk(h)], prl.at[h, k])
            F[far, b, sl, wk(h)] = (
                Pb[far, b, sl, wk(h)].astype(jnp.float32) + R[far, b, sl, wk(h)].astype(jnp.float32)
            ).astype(jnp.bfloat16)

        when(end & who, fn)
        dst = out.at[sl, pl.ds(pl.multiple_of(at + h * half, half), half)]
        src = F.at[far, b, sl, wk(h)]
        if b == 1:
            send(end & who & who, lambda: rc(src, dst, osl.at[h, k], orr.at[idx, 1 + f], (ex, core)))
        else:
            send(end & who & (core != f), lambda: rc(src, dst, osl.at[h, k], orr.at[idx, 0], sib))

            def keep():
                out[sl, pl.ds(pl.multiple_of(at + h * half, half), half)] = F[far, b, sl, wk(h)]

            when(end & who & (core == f), keep)

    units = range(np_)
    sent = len(pending)
    gather(0)
    for b in (3, 2, 1, 0):
        for u in units:
            piece(b, u, 0)
            if b >= 2:
                pass_on(b, u, 0, True)
    for b in (1, 0):
        for u in units:
            settle(b, u, 0, foreign)
    for i, ref in enumerate((mean_out, var_out)):
        when(foreign, lambda i=i, ref=ref: arrived(ref, vr.at[i]))
    for cond, make in pending[:sent]:
        when(cond, lambda make=make: make().wait_send())
    del pending[:sent]
    gather(1)
    for u in units:
        piece(2, u, 1)
        pass_on(2, u, 1, True)
    for u in units:
        piece(3, u, 1)
        pass_on(3, u, 1, native)
        direct(1, 3, u, foreign, (ex + ey - env, core))
    for u in units:
        piece(1, u, 1)
        direct(0, 1, u, native, (ex, core))
        settle(1, u, 1, foreign)
    for u in units:
        piece(0, u, 1)
    for b in (1, 0):
        for u in units:
            settle(b, u, 0, native)
    for u in units:
        settle(0, u, 1, True)
    spot = (far * 4 + y * 2 + 1 - x) * cols + half - core * own_cols
    for u in units:
        def join(u=u):
            sl = pl.ds(u * mt, mt)
            for i in range(2):
                arrived(E.at[i, sl], er.at[i, u])
            out[sl, pl.ds(pl.multiple_of(spot, half), half)] = (
                E[0, sl, :].astype(jnp.float32) + E[1, sl, :].astype(jnp.float32)
            ).astype(jnp.bfloat16)

        when(end & (core == f), join)

    for i in range(nz // 2):
        t = f * (nz // 2) + i
        for src in range(3):
            sf = 1 - f if src == 0 else src - 1
            sx = x if src == 0 else 1 - x
            at = (t * 4 + sf * 2 + sx) * cols - f * own_cols
            halved = end & (t == far) & (y == sf) if src else False
            if src:
                when(halved, lambda at=at, i=i, src=src: arrived(
                    out.at[:, pl.ds(pl.multiple_of(at, half), half)], orr.at[i, src]))
            when(jnp.logical_not(halved) if src else True, lambda at=at, i=i, src=src: arrived(
                out.at[:, pl.ds(pl.multiple_of(at, cols), cols)], orr.at[i, src]))
    for cond, make in pending:
        when(cond, lambda make=make: make().wait_send())


def write_back(pieces, mean, var, logits, mean_out, var_out, out, sems):
    size = out.shape[0] // pieces
    copies = [
        pltpu.make_async_copy(logits.at[pl.ds(i * size, size)], out.at[pl.ds(i * size, size)], sems.at[i])
        for i in range(pieces)
    ]
    copies.append(pltpu.make_async_copy(mean, mean_out, sems.at[pieces]))
    copies.append(pltpu.make_async_copy(var, var_out, sems.at[pieces + 1]))
    for copy in copies:
        copy.start()
    for copy in copies:
        copy.wait()


def f_of_y(y):
    return y


def shards_planes(nz, observations, prior_count, prior_mean, prior_var, policy_weight):
    rows, depth = observations.shape
    cols = policy_weight.shape[1]
    n = lax.axis_size("env")
    own_cols = cols * n // 2
    bf, f32 = jnp.bfloat16, jnp.float32
    dma = pltpu.SemaphoreType.DMA
    vmem = pl.BlockSpec(memory_space=pltpu.VMEM)
    hbm = pl.BlockSpec(memory_space=pl.ANY)
    scratch = [
        pltpu.VMEM((4, rows, depth), bf),
        pltpu.VMEM((4, rows, depth), bf),
        pltpu.VMEM((nz, depth, cols), bf),
        pltpu.VMEM((nz, 4, rows, cols), bf),
        pltpu.VMEM((nz, 2, rows, cols), bf),
        pltpu.VMEM((nz, 2, rows, cols), bf),
        pltpu.VMEM((4 * rows, cols // 2), f32),
        pltpu.VMEM((2, rows, cols // 2), bf),
        pltpu.VMEM((1, depth), jnp.int32),
        pltpu.VMEM((1, depth), f32),
        pltpu.VMEM((1, depth), f32),
        pltpu.VMEM((2, depth), f32),
        pltpu.VMEM((2, depth), f32),
        pltpu.VMEM((2, depth), f32),
        pltpu.VMEM((2, depth), f32),
        pltpu.VMEM((nz, 2, depth), f32),
        pltpu.VMEM((2, depth), f32),
        pltpu.VMEM((2, depth), f32),
        dma((2,)),
        dma((3,)),
        dma((2,)),
        dma((2,)),
        dma((2,)),
        dma((rows // 256,)),
        dma((2, rows // 256)),
        dma((4,)),
        dma((4, 4)),
        dma,
        dma((2,)),
        dma((2,)),
        dma((2,)),
        dma((2,)),
        dma((2, nz - 2, 2)),
        dma((nz, 2)),
        dma((2, 2, CUTS)),
        dma((2,)),
        dma((nz + 1,)),
        dma((nz + 2,)),
        dma,
        dma,
        dma((nz, 2)),
        dma((nz, 2)),
        dma((nz, 2)),
        dma((nz // 2, 3)),
        dma((2, rows // 128)),
        dma((2, rows // 128)),
        dma((2, rows // 128)),
    ]
    row = lambda a: a.reshape(1, depth)
    run_mean, run_var, logits = pl.pallas_call(
        functools.partial(kernel, nz),
        out_shape=(
            pltpu.VMEM((1, depth), f32),
            pltpu.VMEM((1, depth), f32),
            pltpu.VMEM((rows, own_cols), bf),
        ),
        in_specs=[hbm] * 5,
        out_specs=(vmem, vmem, vmem),
        scratch_shapes=scratch,
        compiler_params=pltpu.CompilerParams(
            collective_id=0, has_side_effects=True, vmem_limit_bytes=58 * 1024 * 1024
        ),
    )(observations, row(prior_count), row(prior_mean), row(prior_var), policy_weight)
    pieces = 4
    run_mean, run_var, logits = pl.pallas_call(
        functools.partial(write_back, pieces),
        out_shape=(
            jax.ShapeDtypeStruct((1, depth), f32),
            jax.ShapeDtypeStruct((1, depth), f32),
            jax.ShapeDtypeStruct((rows, own_cols), bf),
        ),
        in_specs=[vmem] * 3,
        out_specs=(hbm,) * 3,
        scratch_shapes=[dma((pieces + 2,))],
    )(*(pltpu.with_memory_space_constraint(a, pltpu.VMEM) for a in (run_mean, run_var, logits)))
    return run_mean.reshape(depth), run_var.reshape(depth), logits


def plane_count(mesh):
    devices = mesh.devices
    if devices.ndim != 2 or devices.shape[1] != 2 or devices.shape[0] % 8:
        return 0
    base = devices[0, 0].coords
    for i in range(devices.shape[0]):
        for j in range(2):
            at = [a - b for a, b in zip(devices[i, j].coords, base)]
            if at != [i % 2, i // 2 % 2, i // 4]:
                return 0
    return devices.shape[0] // 4


def solution(mesh):
    placed = (P("env", "feat"), P("feat"), P("feat"), P("feat"), P("feat", "env"))
    nz = plane_count(mesh)
    body = functools.partial(shards_planes, nz) if nz == 4 else shards_general
    return jax.shard_map(
        body,
        mesh=mesh,
        in_specs=placed,
        out_specs=(P("feat"), P("feat"), P("env", "feat")),
        check_vma=False,
    )
```
